128 devices in a mesh: stream: 16 (over x, z_hi, core), leaf: 8 (over y, z_lo).
Axes of the slice: x: 4, y: 4, z: 4 (z_hi: 2, z_lo: 2; z = z_hi * 2 + z_lo), core: 2. Of those that a mesh axis runs over, the one named last changes fastest.
Arguments:
- points_rhs: bfloat16 [8192, 32, 128], P(('stream', 'leaf')), may hold values from -6 to 6
- leaf_basis: bfloat16 [8192, 64, 128], P(('stream', 'leaf')), may hold values from -0.5 to 0.5
- transfer: bfloat16 [4096, 64, 128], P(('stream', 'leaf')), may hold values from -0.5 to 0.5
- leaf_coupling: bfloat16 [8192, 64, 256], P(('stream', 'leaf')), may hold values from -0.375 to 0.375
- parent_coupling: bfloat16 [4096, 64, 512], P(('stream', 'leaf')), may hold values from -0.25 to 0.25
- near_blocks: bfloat16 [8192, 3, 128, 128], P(('stream', 'leaf')), may hold values from -0.3125 to 0.3125
- near_offsets: int32 [8192, 3], P(('stream', 'leaf')), may hold values from -2 to 2, as said below
- coupling_offsets: int32 [8192, 4], P(('stream', 'leaf')), may hold values from -5 to 5, as said below
- parent_owner: int32 [4096, 8], P(('stream', 'leaf')), may hold values from 0 to 127, all different within a row; in each aligned block of 32 rows (0 to 31, 32 to 63, ...) at most 4 rows name the same one
- parent_local: int32 [4096, 8], P(('stream', 'leaf')), may hold values from 0 to 31
Outputs:
- product: bfloat16 [8192, 32, 128], P(('stream', 'leaf'))
The draws below stay inside these ranges and needn't reach their ends.
Inputs may be any that keep to these rules, and one draw needn't show every extreme that they name: `near_offsets`: each row holds 3 different offsets; the first is 0. `coupling_offsets`: each row holds 4 different nonzero offsets, none of which stands in the same row of near_offsets. `parent_owner`: each row names 8 different blocks; the rows of one device name no block more than 4 times, and in every draw some block is named exactly 4 times by the rows of some device.
All inputs are finite; a program needn't handle non-finite values.
Results may differ from the reference program's by a relative error of at most 0.0053.
Values may be sent and summed in bfloat16 or wider, within the bound.
A program may use at most 128 MiB of HBM per device.

```python
import math
import jax
import jax.numpy as jnp
import numpy as np
from jax import lax

R = 64
NRHS = 32
LS = 128
KN = 3
KC = 4
KP = 8
LEAF_DEV = 64
PAR_DEV = 32
NLEAF = 8192
NPAR = 4096
CAP = 4
DEVICES = 128


def leaf_lists(key):
    key_near = jax.random.fold_in(key, 11)
    key_far = jax.random.fold_in(key, 23)
    near_pool = jnp.array([-2, -1, 1, 2], jnp.int32)
    far_pool = jnp.array([-5, -4, -3, 3, 4, 5], jnp.int32)
    near_scores = jax.random.randint(key_near, (NLEAF, 4), 0, 1 << 20, dtype=jnp.int32) * 16 + jnp.arange(4, dtype=jnp.int32)
    near_order = jnp.argsort(near_scores, axis=1, stable=True)
    chosen = near_pool[near_order]
    near_rows = jnp.concatenate([jnp.zeros((NLEAF, 1), jnp.int32), chosen[:, :KN - 1]], axis=1)
    remaining = jnp.concatenate([chosen[:, KN - 1:], jnp.broadcast_to(far_pool, (NLEAF, 6))], axis=1)
    pool_size = 11 - KN
    far_scores = jax.random.randint(key_far, (NLEAF, pool_size), 0, 1 << 20, dtype=jnp.int32) * 16 + jnp.arange(pool_size, dtype=jnp.int32)
    far_order = jnp.argsort(far_scores, axis=1, stable=True)
    far_rows = jnp.take_along_axis(remaining, far_order, axis=1)[:, :KC]
    return (near_rows, far_rows)


def draw_near_offsets(key, part):
    return leaf_lists(key)[0]


def draw_coupling_offsets(key, part):
    return leaf_lists(key)[1]


def set_ends(entries, key, low, top_value):
    dims = entries.shape
    index_at = [jax.random.randint(jax.random.fold_in(key, axis), (), 0, dims[axis]) for axis in range(len(dims))]
    entries = entries.at[tuple(index_at)].set(low)
    longest = dims.index(max(dims))
    index_at[longest] = (index_at[longest] + 1) % dims[longest]
    return entries.at[tuple(index_at)].set(top_value)


def steps_of(stream_key, shape, pieces, smallest, largest):
    def one(dim, shards_of):
        draws = jax.random.uniform(jax.random.fold_in(jax.random.fold_in(stream_key, 6), dim), (shards_of,), jnp.float32, smallest / len(pieces), largest / len(pieces))
        return jnp.repeat(jnp.exp(draws), shape[dim] // shards_of).reshape((-1,) + (1,) * (len(shape) - dim - 1))

    level = one(*pieces[0])
    for cut in pieces[1:]:
        level = level * one(*cut)
    return level


def deal_out(own_key, own, number, rows, amount, top, bound, skew):
    sequence = jax.random.permutation(own_key, amount)
    crowded, usual = portions_of(amount, rows * top, bound, skew, True), portions_of(amount, rows * top, bound, skew, False)
    places = jnp.arange(amount)

    def named(sizes, turn):
        used = int((sizes > 0).sum())
        fixed = max(1, used // 4)
        moved = fixed + (places - fixed + turn * (used - fixed)) % max(1, amount - fixed)
        return jnp.zeros((amount,), jnp.int32).at[sequence[jnp.where(places < fixed, places, moved)]].set(jnp.asarray(sizes, jnp.int32))

    sizes = jnp.where(number % 4 == 0, named(crowded, number // 4), named(usual, number - number // 4 - 1))
    mixed = jax.random.permutation(jax.random.fold_in(own, 3), amount)
    source_of, taker = mixed[0:amount // 2 * 2:2], mixed[1:amount // 2 * 2:2]
    room = jnp.minimum(sizes[source_of] - 1, bound - sizes[taker]) // 2
    room = jnp.where((source_of == sequence[0]) | (taker == sequence[0]) | (sizes[taker] == 0), 0, jnp.maximum(room, 0))
    moved = jax.random.randint(jax.random.fold_in(own, 4), (amount // 2,), 0, 1 << 20) % (room + 1)
    sizes = sizes.at[source_of].add(-moved).at[taker].add(moved)
    labels = jnp.searchsorted(jnp.cumsum(sizes), jnp.arange(rows * top), side="right").astype(jnp.int32)
    listing = labels.reshape(top, rows).T
    listing = listing[jax.random.permutation(jax.random.fold_in(own, 1), rows)]
    turn = jax.random.randint(jax.random.fold_in(own, 2), (rows, 1), 0, top)
    return jnp.take_along_axis(listing, (jnp.arange(top)[None, :] + turn) % top, axis=1)


def portions_of(amount, total, most, lean, full):
    weights = [(1 << 20) // math.isqrt(rank ** lean) + 1 for rank in range(1, amount + 1)]
    largest = most if full else min(most, max(-(-total // amount), total * weights[0] // sum(weights)))
    least = 1 if total - largest >= amount - 1 else 0
    holding, rest = [largest] + [least] * (amount - 1), total - largest - least * (amount - 1)
    while rest > 0:
        movable = [i for i in range(1, amount) if holding[i] < largest] or [i for i in range(1, amount) if holding[i] < most]
        pool, left = sum([weights[i] for i in movable]), rest
        for i in movable:
            addition = min(most - holding[i], max(1, left * weights[i] // pool), rest)
            holding[i] = holding[i] + addition
            rest = rest - addition
    return np.array(holding)


def scatter_about(rng, shape, spread, reach, shards=(), kind=jnp.bfloat16):
    drawn = spread * jax.random.normal(rng, shape, jnp.float32)
    if shards:
        drawn = drawn * steps_of(rng, shape, shards, -0.22, 0.18)
    return jnp.clip(drawn, -reach, reach).astype(kind)


def setup_inputs(seed: int = 0) -> dict:
    key_list = jax.random.split(jax.random.key(seed), 11)
    points_rhs = scatter_about(key_list[0], (NLEAF, NRHS, LS), 1.0, 6.0, ((0, 128),))
    leaf_basis = scatter_about(key_list[1], (NLEAF, R, LS), LS ** -0.5, 0.5, ((0, 128),))
    transfer = scatter_about(key_list[2], (NPAR, R, 2 * R), (2 * R) ** -0.5, 0.5, ((0, 128),))
    leaf_coupling = scatter_about(key_list[3], (NLEAF, R, KC * R), (KC * R) ** -0.5, 0.375, ((0, 128),))
    parent_coupling = scatter_about(key_list[4], (NPAR, R, KP * R), (KP * R) ** -0.5, 0.25, ((0, 128),))
    near_blocks = scatter_about(key_list[5], (NLEAF, KN, LS, LS), (KN * LS) ** -0.5, 0.3125, ((0, 128),))
    near_offsets = draw_near_offsets(jax.random.fold_in(key_list[10], 71), 0)
    coupling_offsets = draw_coupling_offsets(jax.random.fold_in(key_list[10], 71), 0)
    parent_owner_keys = jax.random.split(jax.random.fold_in(key_list[8], 1), NPAR // PAR_DEV)
    parent_owner_turns = jax.random.permutation(jax.random.fold_in(key_list[8], 3), NPAR // PAR_DEV)
    parent_owner = jax.vmap(lambda own, number: deal_out(jax.random.fold_in(key_list[8], 2), own, number, PAR_DEV, DEVICES, KP, CAP, 1))(parent_owner_keys, parent_owner_turns).reshape((NPAR, KP))
    parent_local = set_ends(jax.random.randint(key_list[9], (NPAR, KP), 0, PAR_DEV), jax.random.fold_in(key_list[9], 1), 0, PAR_DEV - 1).astype(jnp.int32)
    return {"points_rhs": points_rhs, "leaf_basis": leaf_basis, "transfer": transfer, "leaf_coupling": leaf_coupling, "parent_coupling": parent_coupling, "near_blocks": near_blocks, "near_offsets": near_offsets, "coupling_offsets": coupling_offsets, "parent_owner": parent_owner, "parent_local": parent_local}


def shifted_rows(padded, offsets, reach_leaves):
    row_count = offsets.shape[0]
    row_base = jnp.arange(row_count, dtype=jnp.int32)[:, None] + reach_leaves
    return padded[(row_base + offsets).astype(jnp.int32)]


def near_block(paired):
    return jnp.einsum('cknj,ckqj->cnq', paired[0].astype(jnp.float32), paired[1].astype(jnp.float32))


def reference(points_rhs, leaf_basis, transfer, leaf_coupling, parent_coupling, near_blocks, near_offsets, coupling_offsets, parent_owner, parent_local):
    leaf_coeffs = jnp.einsum('cnp,crp->cnr', points_rhs.astype(jnp.float32), leaf_basis.astype(jnp.float32)).astype(jnp.bfloat16)
    paired = leaf_coeffs.reshape(NPAR, 2, NRHS, R).transpose(0, 2, 1, 3).reshape(NPAR, NRHS, 2 * R)
    parent_coeffs = jnp.einsum('pnk,prk->pnr', paired.astype(jnp.float32), transfer.astype(jnp.float32)).astype(jnp.bfloat16)
    coeff_padded = jnp.pad(leaf_coeffs, ((5, 5), (0, 0), (0, 0)))
    sources = shifted_rows(coeff_padded, coupling_offsets, 5)
    coupling_panel = leaf_coupling.reshape(NLEAF, R, KC, R)
    leaf_field = jnp.einsum('cknj,crkj->cnr', sources.astype(jnp.float32), coupling_panel.astype(jnp.float32))
    source_rows = (parent_owner * PAR_DEV + parent_local).astype(jnp.int32)
    remote = parent_coeffs[source_rows]
    parent_panel = parent_coupling.reshape(NPAR, R, KP, R)
    parent_field = jnp.einsum('pknj,prkj->pnr', remote.astype(jnp.float32), parent_panel.astype(jnp.float32))
    parent_half = lax.optimization_barrier(parent_field.astype(jnp.bfloat16))
    downward = jnp.einsum('pnr,prk->pnk', parent_half.astype(jnp.float32), transfer.astype(jnp.float32))
    downward = downward.reshape(NPAR, NRHS, 2, R).transpose(0, 2, 1, 3).reshape(NLEAF, NRHS, R)
    leaf_total = (leaf_field + downward).astype(jnp.bfloat16)
    far_terms = jnp.einsum('cnr,crp->cnp', leaf_total.astype(jnp.float32), leaf_basis.astype(jnp.float32))
    point_padded = jnp.pad(points_rhs, ((2, 2), (0, 0), (0, 0)))
    near_rows = shifted_rows(point_padded, near_offsets, 2).reshape(DEVICES, LEAF_DEV, KN, NRHS, LS)
    block_rows = near_blocks.reshape(DEVICES, LEAF_DEV, KN, LS, LS)
    near_terms = lax.map(near_block, (near_rows, block_rows)).reshape(NLEAF, NRHS, LS)
    return (far_terms + near_terms).astype(jnp.bfloat16)
```

```python
import random

import jax
import jax.numpy as jnp
from jax import lax
from jax.experimental import pallas as pl
from jax.experimental.pallas import tpu as pltpu
from jax.sharding import PartitionSpec as P

MESH = pl.DeviceIdType.MESH
F32 = jnp.float32
BF16 = jnp.bfloat16
I32 = jnp.int32
NDEV = 128
NL = 64
NP = 32
KP = 8
CAP = 4
LAST = (((1,), (1,)), ((), ()))


def send_order():
    offsets = [
        (dx, dy, dz, dc)
        for dx in range(4)
        for dy in range(4)
        for dz in range(4)
        for dc in range(2)
    ][1:]
    random.Random(1).shuffle(offsets)
    hops = lambda o: sum(min(v, 4 - v) for v in o[:3])
    offsets.sort(key=lambda o: -hops(o))
    return offsets


ORDER = send_order()


def dot_last(a, b):
    return lax.dot_general(a, b, LAST, preferred_element_type=F32)


def dot(a, b):
    return jnp.dot(a, b, preferred_element_type=F32)


def kernel(
    points, basis, transfer, leaf_cpl, parent_cpl, near, near_off, cpl_off, owner, local, out,
    pts, bas, tra, lcp, pcp, nea,
    coef, pair_buf, tiles, near_acc, leaf_acc, staged,
    ask, asked, asked_rows, slots_v, ranks,
    send_buf, recv_buf, out_buf,
    asked_s, slots_s,
    in_sems, loc_sem, out_sem, ask_send, ask_recv, halo_send, halo_recv, data_send, data_recv,
):
    s = lax.axis_index("stream")
    l = lax.axis_index("leaf")
    rem = lambda a, b: lax.rem(a, jnp.int32(b))
    div = lambda a, b: lax.div(a, jnp.int32(b))
    core, zh, x, y, zl = rem(s, 2), rem(div(s, 2), 2), div(s, 4), div(l, 2), rem(l, 2)
    z = zh * 2 + zl
    me = s * 8 + l
    xs = [rem(x + i, 4) * 4 for i in range(4)]
    ys = [rem(y + i, 4) * 2 for i in range(4)]
    zs = [rem(z + i, 4) for i in range(4)]
    zhs = [div(v, 2) * 2 for v in zs]
    zls = [rem(v, 2) for v in zs]
    cs = [core, 1 - core]

    def place(o):
        dx, dy, dz, dc = o
        return xs[dx] + zhs[dz] + cs[dc], ys[dy] + zls[dz]

    following = rem(me + 1, NDEV)
    previous = rem(me + NDEV - 1, NDEV)
    next_dev = (div(following, 8), rem(following, 8))
    prev_dev = (div(previous, 8), rem(previous, 8))

    loads = []
    for n, (src, dst) in enumerate((
        (points, pts.at[pl.ds(2, NL)]), (basis, bas), (transfer, tra),
        (near, nea), (leaf_cpl, lcp), (parent_cpl, pcp),
    )):
        c = pltpu.make_async_copy(src, dst, in_sems.at[n])
        c.start()
        loads.append(c)

    barrier = pltpu.get_barrier_semaphore()
    for o in ORDER:
        pl.semaphore_signal(barrier, inc=1, device_id=place(o), device_id_type=MESH)

    lane = lax.broadcasted_iota(I32, (NP, NDEV), 1)
    own = owner[...]
    loc = local[...]
    hits = jnp.zeros((NP, NDEV), I32)
    wanted = jnp.zeros((NP, NDEV), I32)
    for k in range(KP):
        eq = own[:, k:k + 1] == lane
        hits += jnp.where(eq, 1, 0)
        wanted += jnp.where(eq, loc[:, k:k + 1], 0)
    seen = jnp.zeros((1, NDEV), I32)
    rows = [jnp.zeros((1, NDEV), I32) for _ in range(CAP)]
    for p in range(NP):
        ranks[p:p + 1, :] = seen
        hit = hits[p:p + 1, :]
        for q in range(CAP):
            rows[q] = jnp.where((hit > 0) & (seen == q), wanted[p:p + 1, :], rows[q])
        seen = seen + hit
    table = jnp.concatenate(rows + [jnp.zeros((NDEV - CAP, NDEV), I32)], axis=0)
    ask[...] = table.T.reshape(NDEV, 1, NDEV)
    before = ranks[...]
    slot = jnp.zeros((NP, NDEV), I32)
    for k in range(KP):
        eq = own[:, k:k + 1] == lane
        rank = jnp.sum(jnp.where(eq, before, 0), axis=1, keepdims=True)
        slot = jnp.where(lane == k, own[:, k:k + 1] * CAP + rank, slot)
    slots_v[...] = slot
    slot_copy = pltpu.make_async_copy(slots_v, slots_s, loc_sem)
    slot_copy.start()

    for c in loads[:3]:
        c.wait()
    low32 = lax.broadcasted_iota(I32, (32, 128), 1) < 64
    low16 = lax.broadcasted_iota(I32, (16, 128), 1) < 64

    def up_leaf(i, _):
        for u in range(4):
            p = i * 4 + u
            a = pts[pl.ds(2 + 2 * p, 2)].reshape(64, 128)
            b = bas[pl.ds(2 * p, 2)].reshape(128, 128)
            both = dot_last(a, b)
            pair = jnp.where(low32, both[:32], both[32:])
            swap = pltpu.roll(pair, 64, 1)
            pair_buf[p] = pair.astype(BF16)
            coef[5 + 2 * p] = jnp.where(low32, pair, swap).astype(BF16)
            coef[6 + 2 * p] = jnp.where(low32, swap, pair).astype(BF16)
        return 0

    lax.fori_loop(0, NP // 4, up_leaf, 0)

    def up_parent(i, _):
        for u in range(4):
            p = i * 4 + u
            t = tra[p]
            twice = dot_last(pair_buf[p], jnp.concatenate([t, t], axis=0))
            tiles[p] = jnp.where(low16, twice[:16], twice[16:]).astype(BF16)
        return 0

    lax.fori_loop(0, NP // 4, up_parent, 0)

    pl.semaphore_wait(barrier, NDEV - 1)
    for o in ORDER:
        st, lf = place(o)
        pltpu.make_async_remote_copy(
            src_ref=ask.at[st * 8 + lf], dst_ref=asked.at[me], send_sem=ask_send,
            recv_sem=ask_recv, device_id=(st, lf), device_id_type=MESH,
        ).start()
    asked[me] = ask[me]
    halos = []
    for n, (src, dst, dev) in enumerate((
        (pts.at[pl.ds(64, 2)], pts.at[pl.ds(0, 2)], next_dev),
        (pts.at[pl.ds(2, 2)], pts.at[pl.ds(66, 2)], prev_dev),
        (coef.at[pl.ds(64, 5)], coef.at[pl.ds(0, 5)], next_dev),
        (coef.at[pl.ds(5, 5)], coef.at[pl.ds(69, 5)], prev_dev),
    )):
        h = pltpu.make_async_remote_copy(
            src_ref=src, dst_ref=dst, send_sem=halo_send.at[n], recv_sem=halo_recv.at[n],
            device_id=dev, device_id_type=MESH,
        )
        h.start()
        halos.append(h)

    def wait_rows(ref, count, sem):
        part = ref.at[pl.ds(0, count)]
        pltpu.make_async_copy(part, part, sem).wait()

    wait_rows(asked, NDEV - 1, ask_recv)
    wait_rows(ask, NDEV - 1, ask_send)
    asked_rows[...] = asked[...].reshape(NDEV, NDEV).T[:8]
    c = pltpu.make_async_copy(asked_rows, asked_s, loc_sem)
    slot_copy.wait()
    c.start()
    c.wait()

    for n, o in enumerate(ORDER):
        st, lf = place(o)
        to = st * 8 + lf
        for q in range(CAP):
            send_buf[n, q] = tiles[asked_s[q, to]]
        pltpu.make_async_remote_copy(
            src_ref=send_buf.at[n], dst_ref=recv_buf.at[me], send_sem=data_send,
            recv_sem=data_recv, device_id=(st, lf), device_id_type=MESH,
        ).start()
    for q in range(CAP):
        recv_buf[me, q] = tiles[asked_s[q, me]]

    for h in halos:
        h.wait()

    @pl.when(me == 0)
    def _():
        pts[0:2] = jnp.zeros((2, 32, 128), BF16)
        coef[0:5] = jnp.zeros((5, 32, 128), BF16)

    @pl.when(me == NDEV - 1)
    def _():
        pts[66:68] = jnp.zeros((2, 32, 128), BF16)
        coef[69:74] = jnp.zeros((5, 32, 128), BF16)

    loads[3].wait()

    def near_body(i, _):
        for u in range(4):
            c = i * 4 + u
            acc = None
            for k in range(3):
                term = dot_last(pts[c + 2 + near_off[c, k]], nea[c, k])
                acc = term if acc is None else acc + term
            near_acc[c] = acc
        return 0

    lax.fori_loop(0, NL // 4, near_body, 0)
    loads[4].wait()

    def leaf_body(i, _):
        for u in range(4):
            p = i * 4 + u
            w = lcp[pl.ds(2 * p, 2)].reshape(128, 256)
            sides = []
            for j in range(2):
                c = 2 * p + j
                src = [coef[c + 5 + cpl_off[c, k]] for k in range(4)]
                sides.append(jnp.concatenate(
                    [jnp.where(low32, src[0], src[1]), jnp.where(low32, src[2], src[3])], axis=1
                ))
            both = dot_last(jnp.concatenate(sides, axis=0), w)
            leaf_acc[p] = jnp.where(low32, both[:32], both[32:])
        return 0

    lax.fori_loop(0, NP // 4, leaf_body, 0)
    loads[5].wait()

    wait_rows(recv_buf, NDEV - 1, data_recv)

    def stage(i, _):
        for u in range(4):
            p = i * 4 + u
            for m in range(KP // 2):
                va = recv_buf[div(slots_s[p, 2 * m], CAP), rem(slots_s[p, 2 * m], CAP)]
                vb = recv_buf[div(slots_s[p, 2 * m + 1], CAP), rem(slots_s[p, 2 * m + 1], CAP)]
                staged[p, 0:16, m * 128:(m + 1) * 128] = jnp.where(low16, va, pltpu.roll(vb, 64, 1))
                staged[p, 16:32, m * 128:(m + 1) * 128] = jnp.where(low16, pltpu.roll(va, 64, 1), vb)
        return 0

    lax.fori_loop(0, NP // 4, stage, 0)

    def down(i, _):
        ps = [i * 8 + u for u in range(8)]
        halves = [dot_last(staged[p], pcp[p]).astype(BF16) for p in ps]
        downs = [dot(h, tra[p]) for h, p in zip(halves, ps)]
        for p, d in zip(ps, downs):
            total = leaf_acc[p] + d
            zero = jnp.zeros_like(total)
            both = jnp.concatenate(
                [jnp.where(low32, total, zero), jnp.where(low32, zero, total)], axis=0
            ).astype(BF16)
            far = dot(both, bas[pl.ds(2 * p, 2)].reshape(128, 128))
            res = far + near_acc[pl.ds(2 * p, 2)].reshape(64, 128)
            out_buf[pl.ds(2 * p, 2)] = res.astype(BF16).reshape(2, 32, 128)
        return 0

    lax.fori_loop(0, NP // 8, down, 0)
    o = pltpu.make_async_copy(out_buf, out, out_sem)
    o.start()
    wait_rows(send_buf, NDEV - 1, data_send)
    o.wait()


def on_device(*args):
    anywhere = pl.BlockSpec(memory_space=pl.ANY)
    smem = pl.BlockSpec(memory_space=pltpu.SMEM)
    vmem = pl.BlockSpec(memory_space=pltpu.VMEM)
    dma = pltpu.SemaphoreType.DMA
    return pl.pallas_call(
        kernel,
        out_shape=jax.ShapeDtypeStruct((NL, 32, 128), BF16),
        in_specs=[anywhere] * 6 + [smem] * 2 + [vmem] * 2,
        out_specs=anywhere,
        scratch_shapes=[
            pltpu.VMEM((NL + 4, 32, 128), BF16),
            pltpu.VMEM((NL, 64, 128), BF16),
            pltpu.VMEM((NP, 64, 128), BF16),
            pltpu.VMEM((NL, 64, 256), BF16),
            pltpu.VMEM((NP, 64, 512), BF16),
            pltpu.VMEM((NL, 3, 128, 128), BF16),
            pltpu.VMEM((NL + 10, 32, 128), BF16),
            pltpu.VMEM((NP, 32, 128), BF16),
            pltpu.VMEM((NP, 16, 128), BF16),
            pltpu.VMEM((NL, 32, 128), F32),
            pltpu.VMEM((NP, 32, 128), F32),
            pltpu.VMEM((NP, 32, 512), BF16),
            pltpu.VMEM((NDEV, 1, NDEV), I32),
            pltpu.VMEM((NDEV, 1, NDEV), I32),
            pltpu.VMEM((8, NDEV), I32),
            pltpu.VMEM((NP, NDEV), I32),
            pltpu.VMEM((NP, NDEV), I32),
            pltpu.VMEM((NDEV - 1, CAP, 16, 128), BF16),
            pltpu.VMEM((NDEV, CAP, 16, 128), BF16),
            pltpu.VMEM((NL, 32, 128), BF16),
            pltpu.SMEM((8, NDEV), I32),
            pltpu.SMEM((NP, NDEV), I32),
            dma((6,)), dma, dma, dma, dma, dma((4,)), dma((4,)), dma, dma,
        ],
        compiler_params=pltpu.CompilerParams(
            collective_id=0, has_side_effects=True, vmem_limit_bytes=56 * 1024 * 1024
        ),
        name="h2",
    )(*args)


def solution(mesh):
    both = ("stream", "leaf")
    placed = tuple(P(both, *([None] * n)) for n in (2, 2, 2, 2, 2, 3, 1, 1, 1, 1))
    return jax.shard_map(
        on_device, mesh=mesh, in_specs=placed, out_specs=P(both, None, None), check_vma=False
    )
```

```python
import jax
import jax.numpy as jnp
from jax import lax
from jax.experimental import pallas as pl
from jax.experimental.pallas import tpu as pltpu
from jax.sharding import PartitionSpec as P

MESH = pl.DeviceIdType.MESH
F32 = jnp.float32
BF16 = jnp.bfloat16
I32 = jnp.int32
NDEV = 128
NL = 64
NP = 32
KP = 8
CAP = 4
LAST = (((1,), (1,)), ((), ()))


NQ = 4
ROUTES = ((0, 1, 2), (1, 2, 0), (2, 0, 1), (0, 1, 2))
PARTNERS = [(a, d, dc) for a in range(3) for d in (2, 1, 3) for dc in range(2)] + [(0, 0, 1)]


def dot_last(a, b):
    return lax.dot_general(a, b, LAST, preferred_element_type=F32)


def dot(a, b):
    return jnp.dot(a, b, preferred_element_type=F32)


def kernel(*refs):
    held, recv_buf = refs[-8:-4], refs[-4:]
    body(*refs[:-8], held, recv_buf)


def body(
    points, basis, transfer, leaf_cpl, parent_cpl, near, near_off, cpl_off, owner, local, out,
    pts, bas, tra, lcp, pcp, nea,
    coef, pair_buf, near_acc, leaf_acc, staged,
    turned, ask, asked, slots_v, ranks,
    send_buf, out_buf,
    asked_s, slots_s,
    in_sems, slot_sem, asked_sem, out_sem, ask_send, ask_recv, halo_send, halo_recv,
    held_send, first_recv, second_recv, data_send, data_recv,
    held, recv_buf,
):
    s = lax.axis_index("stream")
    l = lax.axis_index("leaf")
    rem = lambda a, b: lax.rem(a, jnp.int32(b))
    div = lambda a, b: lax.div(a, jnp.int32(b))
    core = rem(s, 2)
    at = (div(s, 4), div(l, 2), rem(div(s, 2), 2) * 2 + rem(l, 2))
    me = s * 8 + l

    adds = (
        lambda v: (v * 4, 0),
        lambda v: (0, v * 2),
        lambda v: (div(v, 2) * 2, rem(v, 2)),
    )
    shifted = [[adds[a](rem(at[a] + d, 4)) for d in range(4)] for a in range(3)]

    def place(a, d, dc):
        st = core if dc == 0 else 1 - core
        lf = 0
        for axis in range(3):
            part = shifted[axis][d if axis == a else 0]
            st = st + part[0]
            lf = lf + part[1]
        return st, lf

    following = rem(me + 1, NDEV)
    previous = rem(me + NDEV - 1, NDEV)
    next_dev = (div(following, 8), rem(following, 8))
    prev_dev = (div(previous, 8), rem(previous, 8))

    loads = []
    for n, (src, dst) in enumerate((
        (points, pts.at[pl.ds(2, NL)]), (basis, bas), (transfer, tra),
        (near, nea), (leaf_cpl, lcp), (parent_cpl, pcp),
    )):
        c = pltpu.make_async_copy(src, dst, in_sems.at[n])
        c.start()
        loads.append(c)

    barrier = pltpu.get_barrier_semaphore()
    for to in [place(*p) for p in PARTNERS] + [next_dev, prev_dev]:
        pl.semaphore_signal(barrier, inc=1, device_id=to, device_id_type=MESH)

    turned[...] = jnp.zeros((NDEV, NDEV), I32)
    turned[0:KP, 0:NP] = owner[...]
    turned[KP:2 * KP, 0:NP] = local[...]
    both_t = turned[...].T
    own = both_t[:NP, 0:KP]
    loc = both_t[:NP, KP:2 * KP]
    lane = lax.broadcasted_iota(I32, (NP, NDEV), 1)
    hits = jnp.zeros((NP, NDEV), I32)
    wanted = jnp.zeros((NP, NDEV), I32)
    for k in range(KP):
        eq = own[:, k:k + 1] == lane
        hits += jnp.where(eq, 1, 0)
        wanted += jnp.where(eq, loc[:, k:k + 1], 0)
    seen = jnp.zeros((1, NDEV), I32)
    rows = [jnp.zeros((1, NDEV), I32) for _ in range(CAP)]
    for p in range(NP):
        ranks[p:p + 1, :] = seen
        hit = hits[p:p + 1, :]
        for q in range(CAP):
            rows[q] = jnp.where((hit > 0) & (seen == q), wanted[p:p + 1, :], rows[q])
        seen = seen + hit
    for q in range(CAP):
        ask[q:q + 1, :] = rows[q]
        asked[len(PARTNERS), q:q + 1, :] = rows[q]

    for c in loads[:3]:
        c.wait()
    low32 = lax.broadcasted_iota(I32, (32, 128), 1) < 64
    low8 = lax.broadcasted_iota(I32, (8, 128), 1) < 64
    low4 = lax.broadcasted_iota(I32, (4, 128), 1) < 64

    def up_leaf(i, _):
        for u in range(8):
            p = i * 8 + u
            a = pts[pl.ds(2 + 2 * p, 2)].reshape(64, 128)
            b = bas[pl.ds(2 * p, 2)].reshape(128, 128)
            both = dot_last(a, b)
            pair = jnp.where(low32, both[:32], both[32:])
            swap = pltpu.roll(pair, 64, 1)
            pair_buf[p] = pair.astype(BF16)
            coef[5 + 2 * p] = jnp.where(low32, pair, swap).astype(BF16)
            coef[6 + 2 * p] = jnp.where(low32, swap, pair).astype(BF16)
        return 0

    lax.fori_loop(0, NP // 8, up_leaf, 0)
    block = [at[r[1]] * 4 + at[r[0]] for r in ROUTES]

    def up_parent(i, _):
        for u in range(8):
            p = i * 8 + u
            t = tra[p]
            twice = dot_last(pair_buf[p], jnp.concatenate([t, t], axis=0))
            for q in range(NQ):
                v = twice[8 * q:8 * q + 8]
                held[q][block[q], p] = jnp.where(low8, v, pltpu.roll(v, 4, 0))[:4].astype(BF16)
        return 0

    lax.fori_loop(0, NP // 8, up_parent, 0)

    pl.semaphore_wait(barrier, len(PARTNERS) + 2)

    def pass_on(q, src, axis, d, sem):
        pltpu.make_async_remote_copy(
            src_ref=held[q].at[src], dst_ref=held[q].at[src], send_sem=held_send.at[q],
            recv_sem=sem.at[q],
            device_id=place(axis, d, 0), device_id_type=MESH,
        ).start()

    for q, r in enumerate(ROUTES):
        for d in (1, 3, 2):
            pass_on(q, block[q], r[0], d, first_recv)
    for n, p in enumerate(PARTNERS):
        back = [i for i, o in enumerate(PARTNERS) if o == (p[0], (4 - p[1]) % 4, p[2])][0]
        pltpu.make_async_remote_copy(
            src_ref=ask, dst_ref=asked.at[back], send_sem=ask_send, recv_sem=ask_recv,
            device_id=place(*p), device_id_type=MESH,
        ).start()
    halos = []
    for n, (src, dst, dev) in enumerate((
        (pts.at[pl.ds(64, 2)], pts.at[pl.ds(0, 2)], next_dev),
        (pts.at[pl.ds(2, 2)], pts.at[pl.ds(66, 2)], prev_dev),
        (coef.at[pl.ds(64, 5)], coef.at[pl.ds(0, 5)], next_dev),
        (coef.at[pl.ds(5, 5)], coef.at[pl.ds(69, 5)], prev_dev),
    )):
        h = pltpu.make_async_remote_copy(
            src_ref=src, dst_ref=dst, send_sem=halo_send.at[n], recv_sem=halo_recv.at[n],
            device_id=dev, device_id_type=MESH,
        )
        h.start()
        halos.append(h)
    for q, r in enumerate(ROUTES):
        for d in (1, 3, 2):
            pass_on(q, block[q], r[1], d, second_recv)

    before = ranks[...]
    coords = (own // 32, rem(own // 2, 4), rem(own // 16, 2) * 2 + rem(own, 2))
    own_core = rem(own // 8, 2)
    slot = jnp.zeros((NP, NDEV), I32)
    for k in range(KP):
        eq = own[:, k:k + 1] == lane
        rank = jnp.sum(jnp.where(eq, before, 0), axis=1, keepdims=True)
        for n, r in enumerate(ROUTES[:3]):
            value = (coords[r[2]] * 2 + own_core) * 64 + (coords[r[1]] * 4 + coords[r[0]]) * 4
            slot = jnp.where(lane == n * KP + k, value[:, k:k + 1] + rank, slot)
    slots_v[...] = slot
    slot_copy = pltpu.make_async_copy(slots_v, slots_s, slot_sem)
    slot_copy.start()

    def wait_part(part, sem):
        pltpu.make_async_copy(part, part, sem).wait()

    for q, r in enumerate(ROUTES):
        wait_part(held[q].at[pl.ds(0, 3)], first_recv.at[q])
        for e in (1, 3, 2):
            src = at[r[1]] * 4 + rem(at[r[0]] + e, 4)
            for d in (1, 3, 2):
                pass_on(q, src, r[1], d, second_recv)

    wait_part(asked.at[pl.ds(0, len(PARTNERS))], ask_recv)
    asked_copy = pltpu.make_async_copy(asked, asked_s, asked_sem)
    asked_copy.start()

    for h in halos:
        h.wait()

    @pl.when(me == 0)
    def _():
        pts[0:2] = jnp.zeros((2, 32, 128), BF16)
        coef[0:5] = jnp.zeros((5, 32, 128), BF16)

    @pl.when(me == NDEV - 1)
    def _():
        pts[66:68] = jnp.zeros((2, 32, 128), BF16)
        coef[69:74] = jnp.zeros((5, 32, 128), BF16)

    loads[3].wait()

    def near_body(i, _):
        for u in range(4):
            c = i * 4 + u
            acc = None
            for k in range(3):
                term = dot_last(pts[c + 2 + near_off[k, c]], nea[c, k])
                acc = term if acc is None else acc + term
            near_acc[c] = acc
        return 0

    lax.fori_loop(0, NL // 4, near_body, 0)
    loads[4].wait()

    def leaf_body(i, _):
        for u in range(4):
            p = i * 4 + u
            w = lcp[pl.ds(2 * p, 2)].reshape(128, 256)
            sides = []
            for j in range(2):
                c = 2 * p + j
                src = [coef[c + 5 + cpl_off[k, c]] for k in range(4)]
                sides.append(jnp.concatenate(
                    [jnp.where(low32, src[0], src[1]), jnp.where(low32, src[2], src[3])], axis=1
                ))
            both = dot_last(jnp.concatenate(sides, axis=0), w)
            leaf_acc[p] = jnp.where(low32, both[:32], both[32:])
        return 0

    lax.fori_loop(0, NP // 4, leaf_body, 0)
    loads[5].wait()
    asked_copy.wait()
    slot_copy.wait()

    base = core * 8
    for q, r in enumerate(ROUTES):
        wait_part(held[q].at[pl.ds(0, 12)], second_recv.at[q])
        fixed = adds[r[2]](at[r[2]])
        fixed = base + fixed[0] * 8 + fixed[1]

        def gather(ref, offset, n):
            def some(i, _):
                add2 = adds[r[1]](i)
                for j in range(4):
                    add1 = adds[r[0]](jnp.int32(j))
                    who = fixed + (add1[0] + add2[0]) * 8 + add1[1] + add2[1]
                    for c in range(CAP):
                        ref[offset + (i * 4 + j) * CAP + c] = held[q][
                            i * 4 + j, asked_s[n, c, who]
                        ]
                return 0

            lax.fori_loop(0, 4, some, 0)

        mine = (at[r[2]] * 2 + core) * 64
        line = [(i, p) for i, p in enumerate(PARTNERS) if p[0] == r[2] and p[1]]
        line.append((len(PARTNERS) - 1, PARTNERS[-1]))
        for m, (n, p) in enumerate(line):
            start = (q * 7 + m) * 64
            gather(send_buf, start, n)
            pltpu.make_async_remote_copy(
                src_ref=send_buf.at[pl.ds(start, 64)], dst_ref=recv_buf[q].at[pl.ds(mine, 64)],
                send_sem=data_send, recv_sem=data_recv.at[q],
                device_id=place(r[2], p[1], p[2]), device_id_type=MESH,
            ).start()
        gather(recv_buf[q], mine, len(PARTNERS))

    for q in range(NQ):
        wait_part(recv_buf[q].at[pl.ds(0, 448)], data_recv.at[q])

        def stage(i, _):
            for u in range(4):
                p = i * 4 + u
                for m in range(KP // 2):
                    k = (q % 3) * KP + 2 * m
                    va = recv_buf[q][slots_s[p, k]]
                    vb = recv_buf[q][slots_s[p, k + 1]]
                    cols = slice(m * 128, (m + 1) * 128)
                    staged[p, 8 * q:8 * q + 4, cols] = jnp.where(low4, va, pltpu.roll(vb, 64, 1))
                    staged[p, 8 * q + 4:8 * q + 8, cols] = jnp.where(low4, pltpu.roll(va, 64, 1), vb)
            return 0

        lax.fori_loop(0, NP // 4, stage, 0)

    def down(i, _):
        ps = [i * 8 + u for u in range(8)]
        halves = [dot_last(staged[p], pcp[p]).astype(BF16) for p in ps]
        downs = [dot(h, tra[p]) for h, p in zip(halves, ps)]
        for p, d in zip(ps, downs):
            total = leaf_acc[p] + d
            zero = jnp.zeros_like(total)
            both = jnp.concatenate(
                [jnp.where(low32, total, zero), jnp.where(low32, zero, total)], axis=0
            ).astype(BF16)
            far = dot(both, bas[pl.ds(2 * p, 2)].reshape(128, 128))
            res = far + near_acc[pl.ds(2 * p, 2)].reshape(64, 128)
            out_buf[pl.ds(2 * p, 2)] = res.astype(BF16).reshape(2, 32, 128)
        return 0

    lax.fori_loop(0, NP // 8, down, 0)
    o = pltpu.make_async_copy(out_buf, out, out_sem)
    o.start()
    wait_part(send_buf, data_send)
    for q in range(NQ):
        wait_part(held[q].at[pl.ds(0, 15)], held_send.at[q])
    wait_part(asked.at[pl.ds(0, len(PARTNERS))], ask_send)
    o.wait()


def on_device(*args):
    anywhere = pl.BlockSpec(memory_space=pl.ANY)
    smem = pl.BlockSpec(memory_space=pltpu.SMEM)
    vmem = pl.BlockSpec(memory_space=pltpu.VMEM)
    dma = pltpu.SemaphoreType.DMA
    return pl.pallas_call(
        kernel,
        out_shape=jax.ShapeDtypeStruct((NL, 32, 128), BF16),
        in_specs=[anywhere] * 6 + [smem] * 2 + [vmem] * 2,
        out_specs=anywhere,
        scratch_shapes=[
            pltpu.VMEM((NL + 4, 32, 128), BF16),
            pltpu.VMEM((NL, 64, 128), BF16),
            pltpu.VMEM((NP, 64, 128), BF16),
            pltpu.VMEM((NL, 64, 256), BF16),
            pltpu.VMEM((NP, 64, 512), BF16),
            pltpu.VMEM((NL, 3, 128, 128), BF16),
            pltpu.VMEM((NL + 10, 32, 128), BF16),
            pltpu.VMEM((NP, 32, 128), BF16),
            pltpu.VMEM((NL, 32, 128), F32),
            pltpu.VMEM((NP, 32, 128), F32),
            pltpu.VMEM((NP, 32, 512), BF16),
            pltpu.VMEM((NDEV, NDEV), I32),
            pltpu.VMEM((CAP, NDEV), I32),
            pltpu.VMEM((len(PARTNERS) + 1, CAP, NDEV), I32),
            pltpu.VMEM((NP, NDEV), I32),
            pltpu.VMEM((NP, NDEV), I32),
            pltpu.VMEM((NQ * 7 * 64, 4, 128), BF16),
            pltpu.VMEM((NL, 32, 128), BF16),
            pltpu.SMEM((len(PARTNERS) + 1, CAP, NDEV), I32),
            pltpu.SMEM((NP, NDEV), I32),
            dma((6,)), dma, dma, dma, dma, dma, dma((4,)), dma((4,)),
            dma((NQ,)), dma((NQ,)), dma((NQ,)), dma, dma((NQ,)),
            *[pltpu.VMEM((16, NP, 4, 128), BF16)] * NQ,
            *[pltpu.VMEM((512, 4, 128), BF16)] * NQ,
        ],
        compiler_params=pltpu.CompilerParams(
            collective_id=0, has_side_effects=True, vmem_limit_bytes=56 * 1024 * 1024
        ),
        name="h2",
    )(*args[:6], *[v.T for v in args[6:]])


def solution(mesh):
    both = ("stream", "leaf")
    placed = tuple(P(both, *([None] * n)) for n in (2, 2, 2, 2, 2, 3, 1, 1, 1, 1))
    return jax.shard_map(
        on_device, mesh=mesh, in_specs=placed, out_specs=P(both, None, None), check_vma=False
    )
```

```python
import jax
import jax.numpy as jnp
from jax import lax
from jax.experimental import pallas as pl
from jax.experimental.pallas import tpu as pltpu
from jax.sharding import PartitionSpec as P

MESH = pl.DeviceIdType.MESH
F32 = jnp.float32
BF16 = jnp.bfloat16
I32 = jnp.int32
NDEV = 128
NL = 64
NP = 32
KP = 8
CAP = 4
LAST = (((1,), (1,)), ((), ()))


NQ = 4
ROUTES = ((0, 1, 2), (1, 2, 0), (2, 0, 1), (0, 1, 2))
PARTNERS = [(a, d, dc) for a in range(3) for d in (2, 1, 3) for dc in range(2)] + [(0, 0, 1)]


def dot_last(a, b):
    return lax.dot_general(a, b, LAST, preferred_element_type=F32)


def dot(a, b):
    return jnp.dot(a, b, preferred_element_type=F32)


def kernel(*refs):
    held, recv_buf = refs[-8:-4], refs[-4:]
    body(*refs[:-8], held, recv_buf)


def body(
    points, basis, transfer, leaf_cpl, parent_cpl, near, near_off, cpl_off, owner, local, out,
    pts, bas, tra, lcp, pcp, nea,
    coef, pair_buf, near_acc, leaf_acc, staged,
    turned, ask, asked, slots_v, ranks,
    send_buf, out_buf,
    asked_s, slots_s,
    in_sems, slot_sem, asked_sem, out_sem, ask_send, ask_recv, halo_send, halo_recv,
    held_send, first_recv, second_recv, data_send, data_recv,
    held, recv_buf,
):
    s = lax.axis_index("stream")
    l = lax.axis_index("leaf")
    rem = lambda a, b: lax.rem(a, jnp.int32(b))
    div = lambda a, b: lax.div(a, jnp.int32(b))
    core = rem(s, 2)
    at = (div(s, 4), div(l, 2), rem(div(s, 2), 2) * 2 + rem(l, 2))
    me = s * 8 + l

    adds = (
        lambda v: (v * 4, 0),
        lambda v: (0, v * 2),
        lambda v: (div(v, 2) * 2, rem(v, 2)),
    )
    shifted = [[adds[a](rem(at[a] + d, 4)) for d in range(4)] for a in range(3)]

    def place(a, d, dc):
        st = core if dc == 0 else 1 - core
        lf = 0
        for axis in range(3):
            part = shifted[axis][d if axis == a else 0]
            st = st + part[0]
            lf = lf + part[1]
        return st, lf

    following = rem(me + 1, NDEV)
    previous = rem(me + NDEV - 1, NDEV)
    next_dev = (div(following, 8), rem(following, 8))
    prev_dev = (div(previous, 8), rem(previous, 8))

    loads = []
    for n, (src, dst) in enumerate((
        (points, pts.at[pl.ds(2, NL)]), (basis, bas), (transfer, tra),
        (near, nea), (leaf_cpl, lcp), (parent_cpl, pcp),
    )):
        c = pltpu.make_async_copy(src, dst, in_sems.at[n])
        c.start()
        loads.append(c)

    barrier = pltpu.get_barrier_semaphore()
    for to in [place(*p) for p in PARTNERS] + [next_dev, prev_dev]:
        pl.semaphore_signal(barrier, inc=1, device_id=to, device_id_type=MESH)

    turned[...] = jnp.zeros((NDEV, NDEV), I32)
    turned[0:KP, 0:NP] = owner[...]
    turned[KP:2 * KP, 0:NP] = local[...]
    both_t = turned[...].T
    own = both_t[:NP, 0:KP]
    loc = both_t[:NP, KP:2 * KP]
    lane = lax.broadcasted_iota(I32, (NP, NDEV), 1)
    hits = jnp.zeros((NP, NDEV), I32)
    wanted = jnp.zeros((NP, NDEV), I32)
    for k in range(KP):
        eq = own[:, k:k + 1] == lane
        hits += jnp.where(eq, 1, 0)
        wanted += jnp.where(eq, loc[:, k:k + 1], 0)
    seen = jnp.zeros((1, NDEV), I32)
    rows = [jnp.zeros((1, NDEV), I32) for _ in range(CAP)]
    for p in range(NP):
        ranks[p:p + 1, :] = seen
        hit = hits[p:p + 1, :]
        for q in range(CAP):
            rows[q] = jnp.where((hit > 0) & (seen == q), wanted[p:p + 1, :], rows[q])
        seen = seen + hit
    for q in range(CAP):
        ask[q:q + 1, :] = rows[q]
        asked[len(PARTNERS), q:q + 1, :] = rows[q]

    for c in loads[:3]:
        c.wait()
    low32 = lax.broadcasted_iota(I32, (32, 128), 1) < 64
    low8 = lax.broadcasted_iota(I32, (8, 128), 1) < 64
    low4 = lax.broadcasted_iota(I32, (4, 128), 1) < 64

    def up_leaf(i, _):
        for u in range(8):
            p = i * 8 + u
            a = pts[pl.ds(2 + 2 * p, 2)].reshape(64, 128)
            b = bas[pl.ds(2 * p, 2)].reshape(128, 128)
            both = dot_last(a, b)
            pair = jnp.where(low32, both[:32], both[32:])
            swap = pltpu.roll(pair, 64, 1)
            pair_buf[p] = pair.astype(BF16)
            coef[5 + 2 * p] = jnp.where(low32, pair, swap).astype(BF16)
            coef[6 + 2 * p] = jnp.where(low32, swap, pair).astype(BF16)
        return 0

    lax.fori_loop(0, NP // 8, up_leaf, 0)
    block = [at[r[1]] * 4 + at[r[0]] for r in ROUTES]

    def up_parent(i, _):
        for u in range(8):
            p = i * 8 + u
            t = tra[p]
            twice = dot_last(pair_buf[p], jnp.concatenate([t, t], axis=0))
            for q in range(NQ):
                v = twice[8 * q:8 * q + 8]
                held[q][block[q], p] = jnp.where(low8, v, pltpu.roll(v, 4, 0))[:4].astype(BF16)
        return 0

    lax.fori_loop(0, NP // 8, up_parent, 0)

    pl.semaphore_wait(barrier, len(PARTNERS) + 2)

    def pass_on(q, src, axis, d, sem):
        pltpu.make_async_remote_copy(
            src_ref=held[q].at[src], dst_ref=held[q].at[src], send_sem=held_send.at[q],
            recv_sem=sem.at[q],
            device_id=place(axis, d, 0), device_id_type=MESH,
        ).start()

    for q, r in enumerate(ROUTES):
        for d in (1, 3, 2):
            pass_on(q, block[q], r[0], d, first_recv)
    for n, p in enumerate(PARTNERS):
        back = [i for i, o in enumerate(PARTNERS) if o == (p[0], (4 - p[1]) % 4, p[2])][0]
        pltpu.make_async_remote_copy(
            src_ref=ask, dst_ref=asked.at[back], send_sem=ask_send, recv_sem=ask_recv,
            device_id=place(*p), device_id_type=MESH,
        ).start()
    halos = []
    for n, (src, dst, dev) in enumerate((
        (pts.at[pl.ds(64, 2)], pts.at[pl.ds(0, 2)], next_dev),
        (pts.at[pl.ds(2, 2)], pts.at[pl.ds(66, 2)], prev_dev),
        (coef.at[pl.ds(64, 5)], coef.at[pl.ds(0, 5)], next_dev),
        (coef.at[pl.ds(5, 5)], coef.at[pl.ds(69, 5)], prev_dev),
    )):
        h = pltpu.make_async_remote_copy(
            src_ref=src, dst_ref=dst, send_sem=halo_send.at[n], recv_sem=halo_recv.at[n],
            device_id=dev, device_id_type=MESH,
        )
        h.start()
        halos.append(h)
    for q, r in enumerate(ROUTES):
        for d in (1, 3, 2):
            pass_on(q, block[q], r[1], d, second_recv)

    before = ranks[...]
    coords = (own // 32, rem(own // 2, 4), rem(own // 16, 2) * 2 + rem(own, 2))
    own_core = rem(own // 8, 2)
    slot = jnp.zeros((NP, NDEV), I32)
    for k in range(KP):
        eq = own[:, k:k + 1] == lane
        rank = jnp.sum(jnp.where(eq, before, 0), axis=1, keepdims=True)
        for n, r in enumerate(ROUTES):
            value = (coords[r[2]] * 2 + own_core) * 64 + (coords[r[1]] * 4 + coords[r[0]]) * 4
            slot = jnp.where(lane == n * KP + k, value[:, k:k + 1] + rank, slot)
    slots_v[...] = slot
    slot_copy = pltpu.make_async_copy(slots_v, slots_s, slot_sem)
    slot_copy.start()

    def wait_part(part, sem):
        pltpu.make_async_copy(part, part, sem).wait()

    for q, r in enumerate(ROUTES):
        wait_part(held[q].at[pl.ds(0, 3)], first_recv.at[q])
        for e in (1, 3, 2):
            src = at[r[1]] * 4 + rem(at[r[0]] + e, 4)
            for d in (1, 3, 2):
                pass_on(q, src, r[1], d, second_recv)

    wait_part(asked.at[pl.ds(0, len(PARTNERS))], ask_recv)
    asked_copy = pltpu.make_async_copy(asked, asked_s, asked_sem)
    asked_copy.start()

    loads[5].wait()
    asked_copy.wait()
    slot_copy.wait()

    base = core * 8
    for q, r in enumerate(ROUTES):
        wait_part(held[q].at[pl.ds(0, 12)], second_recv.at[q])
        fixed = adds[r[2]](at[r[2]])
        fixed = base + fixed[0] * 8 + fixed[1]

        def gather(ref, offset, n):
            def some(i, _):
                add2 = adds[r[1]](i)
                for j in range(4):
                    add1 = adds[r[0]](jnp.int32(j))
                    who = fixed + (add1[0] + add2[0]) * 8 + add1[1] + add2[1]
                    for c in range(CAP):
                        ref[offset + (i * 4 + j) * CAP + c] = held[q][
                            i * 4 + j, asked_s[n, c, who]
                        ]
                return 0

            lax.fori_loop(0, 4, some, 0)

        mine = (at[r[2]] * 2 + core) * 64
        line = [(i, p) for i, p in enumerate(PARTNERS) if p[0] == r[2] and p[1]]
        line.append((len(PARTNERS) - 1, PARTNERS[-1]))
        for m, (n, p) in enumerate(line):
            start = (q * 7 + m) * 64
            gather(send_buf, start, n)
            pltpu.make_async_remote_copy(
                src_ref=send_buf.at[pl.ds(start, 64)], dst_ref=recv_buf[q].at[pl.ds(mine, 64)],
                send_sem=data_send, recv_sem=data_recv.at[q],
                device_id=place(r[2], p[1], p[2]), device_id_type=MESH,
            ).start()
        gather(recv_buf[q], mine, len(PARTNERS))

    for h in halos:
        h.wait()

    @pl.when(me == 0)
    def _():
        pts[0:2] = jnp.zeros((2, 32, 128), BF16)
        coef[0:5] = jnp.zeros((5, 32, 128), BF16)

    @pl.when(me == NDEV - 1)
    def _():
        pts[66:68] = jnp.zeros((2, 32, 128), BF16)
        coef[69:74] = jnp.zeros((5, 32, 128), BF16)

    loads[3].wait()

    def near_body(i, _):
        for u in range(4):
            c = i * 4 + u
            acc = None
            for k in range(3):
                term = dot_last(pts[c + 2 + near_off[k, c]], nea[c, k])
                acc = term if acc is None else acc + term
            near_acc[c] = acc
        return 0

    lax.fori_loop(0, NL // 4, near_body, 0)
    loads[4].wait()

    def leaf_body(i, _):
        for u in range(4):
            p = i * 4 + u
            w = lcp[pl.ds(2 * p, 2)].reshape(128, 256)
            sides = []
            for j in range(2):
                c = 2 * p + j
                src = [coef[c + 5 + cpl_off[k, c]] for k in range(4)]
                sides.append(jnp.concatenate(
                    [jnp.where(low32, src[0], src[1]), jnp.where(low32, src[2], src[3])], axis=1
                ))
            both = dot_last(jnp.concatenate(sides, axis=0), w)
            leaf_acc[p] = jnp.where(low32, both[:32], both[32:])
        return 0

    lax.fori_loop(0, NP // 4, leaf_body, 0)
    for q in range(NQ):
        wait_part(recv_buf[q].at[pl.ds(0, 448)], data_recv.at[q])

        def stage(i, _):
            for u in range(8):
                p = i * 8 + u
                for m in range(KP // 2):
                    k = q * KP + 2 * m
                    va = recv_buf[q][slots_s[p, k]]
                    vb = recv_buf[q][slots_s[p, k + 1]]
                    cols = slice(m * 128, (m + 1) * 128)
                    staged[p, 8 * q:8 * q + 4, cols] = jnp.where(low4, va, pltpu.roll(vb, 64, 1))
                    staged[p, 8 * q + 4:8 * q + 8, cols] = jnp.where(low4, pltpu.roll(va, 64, 1), vb)
            return 0

        lax.fori_loop(0, NP // 8, stage, 0)

    def down(i, _):
        ps = [i * 16 + u for u in range(16)]
        halves = [dot_last(staged[p], pcp[p]).astype(BF16) for p in ps]
        downs = [dot(h, tra[p]) for h, p in zip(halves, ps)]
        for p, d in zip(ps, downs):
            total = leaf_acc[p] + d
            zero = jnp.zeros_like(total)
            both = jnp.concatenate(
                [jnp.where(low32, total, zero), jnp.where(low32, zero, total)], axis=0
            ).astype(BF16)
            far = dot(both, bas[pl.ds(2 * p, 2)].reshape(128, 128))
            res = far + near_acc[pl.ds(2 * p, 2)].reshape(64, 128)
            out[pl.ds(2 * p, 2)] = res.astype(BF16).reshape(2, 32, 128)
        return 0

    lax.fori_loop(0, NP // 16, down, 0)
    wait_part(send_buf, data_send)
    for q in range(NQ):
        wait_part(held[q].at[pl.ds(0, 15)], held_send.at[q])
    wait_part(asked.at[pl.ds(0, len(PARTNERS))], ask_send)


def on_device(*args):
    anywhere = pl.BlockSpec(memory_space=pl.ANY)
    smem = pl.BlockSpec(memory_space=pltpu.SMEM)
    vmem = pl.BlockSpec(memory_space=pltpu.VMEM)
    dma = pltpu.SemaphoreType.DMA
    return pl.pallas_call(
        kernel,
        out_shape=jax.ShapeDtypeStruct((NL, 32, 128), BF16),
        in_specs=[anywhere]*6 + [smem] * 2 + [vmem] * 2,
        out_specs=vmem,
        scratch_shapes=[
            pltpu.VMEM((NL + 4, 32, 128), BF16),
            pltpu.VMEM((NL, 64, 128), BF16),
            pltpu.VMEM((NP, 64, 128), BF16),
            pltpu.VMEM((NL, 64, 256), BF16),
            pltpu.VMEM((NP, 64, 512), BF16),
            pltpu.VMEM((NL, 3, 128, 128), BF16),
            pltpu.VMEM((NL + 10, 32, 128), BF16),
            pltpu.VMEM((NP, 32, 128), BF16),
            pltpu.VMEM((NL, 32, 128), F32),
            pltpu.VMEM((NP, 32, 128), F32),
            pltpu.VMEM((NP, 32, 512), BF16),
            pltpu.VMEM((NDEV, NDEV), I32),
            pltpu.VMEM((CAP, NDEV), I32),
            pltpu.VMEM((len(PARTNERS) + 1, CAP, NDEV), I32),
            pltpu.VMEM((NP, NDEV), I32),
            pltpu.VMEM((NP, NDEV), I32),
            pltpu.VMEM((NQ * 7 * 64, 4, 128), BF16),
            pltpu.VMEM((NL, 32, 128), BF16),
            pltpu.SMEM((len(PARTNERS) + 1, CAP, NDEV), I32),
            pltpu.SMEM((NP, NDEV), I32),
            dma((6,)), dma, dma, dma, dma, dma, dma((4,)), dma((4,)),
            dma((NQ,)), dma((NQ,)), dma((NQ,)), dma, dma((NQ,)),
            *[pltpu.VMEM((16, NP, 4, 128), BF16)] * NQ,
            *[pltpu.VMEM((512, 4, 128), BF16)] * NQ,
        ],
        compiler_params=pltpu.CompilerParams(
            collective_id=0, has_side_effects=True, vmem_limit_bytes=48 * 1024 * 1024
        ),
        name="h2",
    )(*[pltpu.with_memory_space_constraint(a, pltpu.HBM) for a in args[:6] + tuple(v.T for v in args[6:])])


def solution(mesh):
    both = ("stream", "leaf")
    placed = tuple(P(both, *([None] * n)) for n in (2, 2, 2, 2, 2, 3, 1, 1, 1, 1))
    return jax.shard_map(
        on_device, mesh=mesh, in_specs=placed, out_specs=P(both, None, None), check_vma=False
    )
```

```python
import jax
import jax.numpy as jnp
from jax import lax
from jax.experimental import pallas as pl
from jax.experimental.pallas import tpu as pltpu
from jax.sharding import PartitionSpec as P

MESH = pl.DeviceIdType.MESH
F32 = jnp.float32
BF16 = jnp.bfloat16
I32 = jnp.int32
NDEV = 128
NL = 64
NP = 32
KP = 8
CAP = 4
LAST = (((1,), (1,)), ((), ()))


NQ = 4
ROUTES = ((0, 1, 2), (1, 2, 0), (2, 0, 1), (0, 1, 2))
PARTNERS = [(a, d, dc) for a in range(3) for d in (2, 1, 3) for dc in range(2)] + [(0, 0, 1)]


def dot_last(a, b):
    return lax.dot_general(a, b, LAST, preferred_element_type=F32)


def dot(a, b):
    return jnp.dot(a, b, preferred_element_type=F32)


def kernel(*refs):
    held, recv_buf = refs[-8:-4], refs[-4:]
    body(*refs[:-8], held, recv_buf)


def body(
    points, basis, transfer, leaf_cpl, parent_cpl, near, near_off, cpl_off, owner, local, out,
    pts, bas, tra, lcp, pcp, nea,
    coef, pair_buf, near_acc, leaf_acc, staged,
    turned, ask, asked, slots_v, ranks,
    send_buf, out_buf,
    asked_s, slots_s,
    in_sems, slot_sem, asked_sem, out_sem, ask_send, ask_recv, halo_send, halo_recv,
    held_send, first_recv, second_recv, data_send, data_recv,
    held, recv_buf,
):
    s = lax.axis_index("stream")
    l = lax.axis_index("leaf")
    rem = lambda a, b: lax.rem(a, jnp.int32(b))
    div = lambda a, b: lax.div(a, jnp.int32(b))
    core = rem(s, 2)
    at = (div(s, 4), div(l, 2), rem(div(s, 2), 2) * 2 + rem(l, 2))
    me = s * 8 + l

    adds = (
        lambda v: (v * 4, 0),
        lambda v: (0, v * 2),
        lambda v: (div(v, 2) * 2, rem(v, 2)),
    )
    shifted = [[adds[a](rem(at[a] + d, 4)) for d in range(4)] for a in range(3)]

    def place(a, d, dc):
        st = core if dc == 0 else 1 - core
        lf = 0
        for axis in range(3):
            part = shifted[axis][d if axis == a else 0]
            st = st + part[0]
            lf = lf + part[1]
        return st, lf

    following = rem(me + 1, NDEV)
    previous = rem(me + NDEV - 1, NDEV)
    next_dev = (div(following, 8), rem(following, 8))
    prev_dev = (div(previous, 8), rem(previous, 8))

    loads = []
    for n, (src, dst) in enumerate((
        (points, pts.at[pl.ds(2, NL)]), (basis, bas), (transfer, tra),
        (near, nea), (leaf_cpl, lcp), (parent_cpl, pcp),
    )):
        c = pltpu.make_async_copy(src, dst, in_sems.at[n])
        loads.append(c)
    for c in loads[:3]:
        c.start()

    barrier = pltpu.get_barrier_semaphore()
    for p in PARTNERS:
        pl.semaphore_signal(barrier, inc=1, device_id=place(*p), device_id_type=MESH)

    turned[...] = jnp.zeros((NDEV, NDEV), I32)
    turned[0:KP, 0:NP] = owner[...]
    turned[KP:2 * KP, 0:NP] = local[...]
    both_t = turned[...].T
    own = both_t[:NP, 0:KP]
    loc = both_t[:NP, KP:2 * KP]
    lane = lax.broadcasted_iota(I32, (NP, NDEV), 1)
    hits = jnp.zeros((NP, NDEV), I32)
    wanted = jnp.zeros((NP, NDEV), I32)
    for k in range(KP):
        eq = own[:, k:k + 1] == lane
        hits += jnp.where(eq, 1, 0)
        wanted += jnp.where(eq, loc[:, k:k + 1], 0)
    seen = jnp.zeros((1, NDEV), I32)
    rows = [jnp.zeros((1, NDEV), I32) for _ in range(CAP)]
    for p in range(NP):
        ranks[p:p + 1, :] = seen
        hit = hits[p:p + 1, :]
        for q in range(CAP):
            rows[q] = jnp.where((hit > 0) & (seen == q), wanted[p:p + 1, :], rows[q])
        seen = seen + hit
    for q in range(CAP):
        ask[q:q + 1, :] = rows[q]
        asked[len(PARTNERS), q:q + 1, :] = rows[q]

    for c in loads[:3]:
        c.wait()
    for c in loads[3:]:
        c.start()
    low32 = lax.broadcasted_iota(I32, (32, 128), 1) < 64
    low8 = lax.broadcasted_iota(I32, (8, 128), 1) < 64
    low4 = lax.broadcasted_iota(I32, (4, 128), 1) < 64

    def up_leaf(i, _):
        for u in range(8):
            p = i * 8 + u
            a = pts[pl.ds(2 + 2 * p, 2)].reshape(64, 128)
            b = bas[pl.ds(2 * p, 2)].reshape(128, 128)
            both = dot_last(a, b)
            pair = jnp.where(low32, both[:32], both[32:])
            swap = pltpu.roll(pair, 64, 1)
            pair_buf[p] = pair.astype(BF16)
            coef[5 + 2 * p] = jnp.where(low32, pair, swap).astype(BF16)
            coef[6 + 2 * p] = jnp.where(low32, swap, pair).astype(BF16)
        return 0

    lax.fori_loop(0, NP // 8, up_leaf, 0)
    block = [at[r[1]] * 4 + at[r[0]] for r in ROUTES]

    def up_parent(i, _):
        for u in range(8):
            p = i * 8 + u
            t = tra[p]
            twice = dot_last(pair_buf[p], jnp.concatenate([t, t], axis=0))
            for q in range(NQ):
                v = twice[8 * q:8 * q + 8]
                held[q][block[q], p] = jnp.where(low8, v, pltpu.roll(v, 4, 0))[:4].astype(BF16)
        return 0

    lax.fori_loop(0, NP // 8, up_parent, 0)

    pl.semaphore_wait(barrier, len(PARTNERS))

    def pass_on(q, src, axis, d, sem):
        pltpu.make_async_remote_copy(
            src_ref=held[q].at[src], dst_ref=held[q].at[src], send_sem=held_send.at[q],
            recv_sem=sem.at[q],
            device_id=place(axis, d, 0), device_id_type=MESH,
        ).start()

    for q, r in enumerate(ROUTES):
        for d in (1, 3, 2):
            pass_on(q, block[q], r[0], d, first_recv)
    for n, p in enumerate(PARTNERS):
        back = [i for i, o in enumerate(PARTNERS) if o == (p[0], (4 - p[1]) % 4, p[2])][0]
        pltpu.make_async_remote_copy(
            src_ref=ask, dst_ref=asked.at[back], send_sem=ask_send, recv_sem=ask_recv,
            device_id=place(*p), device_id_type=MESH,
        ).start()
    for q, r in enumerate(ROUTES):
        for d in (1, 3, 2):
            pass_on(q, block[q], r[1], d, second_recv)

    before = ranks[...]
    coords = (own // 32, rem(own // 2, 4), rem(own // 16, 2) * 2 + rem(own, 2))
    own_core = rem(own // 8, 2)
    slot = jnp.zeros((NP, NDEV), I32)
    for k in range(KP):
        eq = own[:, k:k + 1] == lane
        rank = jnp.sum(jnp.where(eq, before, 0), axis=1, keepdims=True)
        for n, r in enumerate(ROUTES):
            value = (coords[r[2]] * 2 + own_core) * 64 + (coords[r[1]] * 4 + coords[r[0]]) * 4
            slot = jnp.where(lane == n * KP + k, value[:, k:k + 1] + rank, slot)
    slots_v[...] = slot
    slot_copy = pltpu.make_async_copy(slots_v, slots_s, slot_sem)
    slot_copy.start()

    def wait_part(part, sem):
        pltpu.make_async_copy(part, part, sem).wait()

    for q, r in enumerate(ROUTES):
        wait_part(held[q].at[pl.ds(0, 3)], first_recv.at[q])
        for e in (1, 3, 2):
            src = at[r[1]] * 4 + rem(at[r[0]] + e, 4)
            for d in (1, 3, 2):
                pass_on(q, src, r[1], d, second_recv)

    wait_part(asked.at[pl.ds(0, len(PARTNERS))], ask_recv)
    asked_copy = pltpu.make_async_copy(asked, asked_s, asked_sem)
    asked_copy.start()

    loads[5].wait()
    asked_copy.wait()
    slot_copy.wait()

    base = core * 8
    halos = []
    for q, r in enumerate(ROUTES):
        wait_part(held[q].at[pl.ds(0, 12)], second_recv.at[q])
        if q == 0:
            for n, (src, dst, dev) in enumerate((
                (pts.at[pl.ds(64, 2)], pts.at[pl.ds(0, 2)], next_dev),
                (pts.at[pl.ds(2, 2)], pts.at[pl.ds(66, 2)], prev_dev),
                (coef.at[pl.ds(64, 5)], coef.at[pl.ds(0, 5)], next_dev),
                (coef.at[pl.ds(5, 5)], coef.at[pl.ds(69, 5)], prev_dev),
            )):
                h = pltpu.make_async_remote_copy(
                    src_ref=src, dst_ref=dst, send_sem=halo_send.at[n], recv_sem=halo_recv.at[n],
                    device_id=dev, device_id_type=MESH,
                )
                h.start()
                halos.append(h)
        fixed = adds[r[2]](at[r[2]])
        fixed = base + fixed[0] * 8 + fixed[1]

        def gather(ref, offset, n):
            def some(i, _):
                add2 = adds[r[1]](i)
                for j in range(4):
                    add1 = adds[r[0]](jnp.int32(j))
                    who = fixed + (add1[0] + add2[0]) * 8 + add1[1] + add2[1]
                    for c in range(CAP):
                        ref[offset + (i * 4 + j) * CAP + c] = held[q][
                            i * 4 + j, asked_s[n, c, who]
                        ]
                return 0

            lax.fori_loop(0, 4, some, 0)

        mine = (at[r[2]] * 2 + core) * 64
        line = [(i, p) for i, p in enumerate(PARTNERS) if p[0] == r[2] and p[1]]
        line.append((len(PARTNERS) - 1, PARTNERS[-1]))
        for m, (n, p) in enumerate(line):
            start = (q * 7 + m) * 64
            gather(send_buf, start, n)
            pltpu.make_async_remote_copy(
                src_ref=send_buf.at[pl.ds(start, 64)], dst_ref=recv_buf[q].at[pl.ds(mine, 64)],
                send_sem=data_send, recv_sem=data_recv.at[q],
                device_id=place(r[2], p[1], p[2]), device_id_type=MESH,
            ).start()
        gather(recv_buf[q], mine, len(PARTNERS))

    for h in halos:
        h.wait()

    @pl.when(me == 0)
    def _():
        pts[0:2] = jnp.zeros((2, 32, 128), BF16)
        coef[0:5] = jnp.zeros((5, 32, 128), BF16)

    @pl.when(me == NDEV - 1)
    def _():
        pts[66:68] = jnp.zeros((2, 32, 128), BF16)
        coef[69:74] = jnp.zeros((5, 32, 128), BF16)

    loads[3].wait()

    def near_body(i, _):
        for u in range(4):
            c = i * 4 + u
            acc = None
            for k in range(3):
                term = dot_last(pts[c + 2 + near_off[k, c]], nea[c, k])
                acc = term if acc is None else acc + term
            near_acc[c] = acc
        return 0

    lax.fori_loop(0, NL // 4, near_body, 0)
    loads[4].wait()

    def leaf_body(i, _):
        for u in range(4):
            p = i * 4 + u
            w = lcp[pl.ds(2 * p, 2)].reshape(128, 256)
            sides = []
            for j in range(2):
                c = 2 * p + j
                src = [coef[c + 5 + cpl_off[k, c]] for k in range(4)]
                sides.append(jnp.concatenate(
                    [jnp.where(low32, src[0], src[1]), jnp.where(low32, src[2], src[3])], axis=1
                ))
            both = dot_last(jnp.concatenate(sides, axis=0), w)
            leaf_acc[p] = jnp.where(low32, both[:32], both[32:])
        return 0

    lax.fori_loop(0, NP // 4, leaf_body, 0)
    for q in range(NQ):
        wait_part(recv_buf[q].at[pl.ds(0, 448)], data_recv.at[q])

        def stage(i, _):
            for u in range(8):
                p = i * 8 + u
                for m in range(KP // 2):
                    k = q * KP + 2 * m
                    va = recv_buf[q][slots_s[p, k]]
                    vb = recv_buf[q][slots_s[p, k + 1]]
                    cols = slice(m * 128, (m + 1) * 128)
                    staged[p, 8 * q:8 * q + 4, cols] = jnp.where(low4, va, pltpu.roll(vb, 64, 1))
                    staged[p, 8 * q + 4:8 * q + 8, cols] = jnp.where(low4, pltpu.roll(va, 64, 1), vb)
            return 0

        lax.fori_loop(0, NP // 8, stage, 0)

    def down(i, _):
        ps = [i * 16 + u for u in range(16)]
        halves = [dot_last(staged[p], pcp[p]).astype(BF16) for p in ps]
        downs = [dot(h, tra[p]) for h, p in zip(halves, ps)]
        for p, d in zip(ps, downs):
            total = leaf_acc[p] + d
            zero = jnp.zeros_like(total)
            both = jnp.concatenate(
                [jnp.where(low32, total, zero), jnp.where(low32, zero, total)], axis=0
            ).astype(BF16)
            far = dot(both, bas[pl.ds(2 * p, 2)].reshape(128, 128))
            res = far + near_acc[pl.ds(2 * p, 2)].reshape(64, 128)
            out[pl.ds(2 * p, 2)] = res.astype(BF16).reshape(2, 32, 128)
        return 0

    lax.fori_loop(0, NP // 16, down, 0)
    wait_part(send_buf, data_send)
    for q in range(NQ):
        wait_part(held[q].at[pl.ds(0, 15)], held_send.at[q])
    wait_part(asked.at[pl.ds(0, len(PARTNERS))], ask_send)


def on_device(*args):
    anywhere = pl.BlockSpec(memory_space=pl.ANY)
    smem = pl.BlockSpec(memory_space=pltpu.SMEM)
    vmem = pl.BlockSpec(memory_space=pltpu.VMEM)
    dma = pltpu.SemaphoreType.DMA
    return pl.pallas_call(
        kernel,
        out_shape=jax.ShapeDtypeStruct((NL, 32, 128), BF16),
        in_specs=[anywhere]*6 + [smem] * 2 + [vmem] * 2,
        out_specs=vmem,
        scratch_shapes=[
            pltpu.VMEM((NL + 4, 32, 128), BF16),
            pltpu.VMEM((NL, 64, 128), BF16),
            pltpu.VMEM((NP, 64, 128), BF16),
            pltpu.VMEM((NL, 64, 256), BF16),
            pltpu.VMEM((NP, 64, 512), BF16),
            pltpu.VMEM((NL, 3, 128, 128), BF16),
            pltpu.VMEM((NL + 10, 32, 128), BF16),
            pltpu.VMEM((NP, 32, 128), BF16),
            pltpu.VMEM((NL, 32, 128), F32),
            pltpu.VMEM((NP, 32, 128), F32),
            pltpu.VMEM((NP, 32, 512), BF16),
            pltpu.VMEM((NDEV, NDEV), I32),
            pltpu.VMEM((CAP, NDEV), I32),
            pltpu.VMEM((len(PARTNERS) + 1, CAP, NDEV), I32),
            pltpu.VMEM((NP, NDEV), I32),
            pltpu.VMEM((NP, NDEV), I32),
            pltpu.VMEM((NQ * 7 * 64, 4, 128), BF16),
            pltpu.VMEM((NL, 32, 128), BF16),
            pltpu.SMEM((len(PARTNERS) + 1, CAP, NDEV), I32),
            pltpu.SMEM((NP, NDEV), I32),
            dma((6,)), dma, dma, dma, dma, dma, dma((4,)), dma((4,)),
            dma((NQ,)), dma((NQ,)), dma((NQ,)), dma, dma((NQ,)),
            *[pltpu.VMEM((16, NP, 4, 128), BF16)] * NQ,
            *[pltpu.VMEM((512, 4, 128), BF16)] * NQ,
        ],
        compiler_params=pltpu.CompilerParams(
            collective_id=0, has_side_effects=True, vmem_limit_bytes=48 * 1024 * 1024
        ),
        name="h2",
    )(*[pltpu.with_memory_space_constraint(a, pltpu.HBM) for a in args[:6] + tuple(v.T for v in args[6:])])


def solution(mesh):
    both = ("stream", "leaf")
    placed = tuple(P(both, *([None] * n)) for n in (2, 2, 2, 2, 2, 3, 1, 1, 1, 1))
    return jax.shard_map(
        on_device, mesh=mesh, in_specs=placed, out_specs=P(both, None, None), check_vma=False
    )
```

```python
import jax
import jax.numpy as jnp
from jax import lax
from jax.experimental import pallas as pl
from jax.experimental.pallas import tpu as pltpu
from jax.sharding import PartitionSpec as P

MESH = pl.DeviceIdType.MESH
F32 = jnp.float32
BF16 = jnp.bfloat16
I32 = jnp.int32
NDEV = 128
NL = 64
NP = 32
KP = 8
CAP = 4
LAST = (((1,), (1,)), ((), ()))


NQ = 4
ROUTES = ((0, 1, 2), (1, 2, 0), (2, 0, 1), (0, 1, 2))
PARTNERS = [(a, d, dc) for a in range(3) for d in (2, 1, 3) for dc in range(2)] + [(0, 0, 1)]


def dot_last(a, b):
    return lax.dot_general(a, b, LAST, preferred_element_type=F32)


def dot(a, b):
    return jnp.dot(a, b, preferred_element_type=F32)


def kernel(*refs):
    held, recv_buf = refs[-8:-4], refs[-4:]
    body(*refs[:-8], held, recv_buf)


def body(
    points, basis, transfer, leaf_cpl, parent_cpl, near, near_off, cpl_off, owner, local, out,
    pts, bas, tra, lcp, pcp, nea,
    coef, pair_buf, near_acc, leaf_acc, staged,
    turned, ask, asked, slots_v, ranks,
    send_buf, out_buf,
    asked_s, slots_s,
    in_sems, slot_sem, asked_sem, out_sem, ask_send, ask_recv, halo_send, halo_recv,
    held_send, first_recv, second_recv, data_send, data_recv,
    held, recv_buf,
):
    s = lax.axis_index("stream")
    l = lax.axis_index("leaf")
    rem = lambda a, b: lax.rem(a, jnp.int32(b))
    div = lambda a, b: lax.div(a, jnp.int32(b))
    core = rem(s, 2)
    at = (div(s, 4), div(l, 2), rem(div(s, 2), 2) * 2 + rem(l, 2))
    me = s * 8 + l

    adds = (
        lambda v: (v * 4, 0),
        lambda v: (0, v * 2),
        lambda v: (div(v, 2) * 2, rem(v, 2)),
    )
    shifted = [[adds[a](rem(at[a] + d, 4)) for d in range(4)] for a in range(3)]

    def place(a, d, dc):
        st = core if dc == 0 else 1 - core
        lf = 0
        for axis in range(3):
            part = shifted[axis][d if axis == a else 0]
            st = st + part[0]
            lf = lf + part[1]
        return st, lf

    following = rem(me + 1, NDEV)
    previous = rem(me + NDEV - 1, NDEV)
    next_dev = (div(following, 8), rem(following, 8))
    prev_dev = (div(previous, 8), rem(previous, 8))

    loads = []
    for n, (src, dst) in enumerate((
        (points, pts.at[pl.ds(2, NL)]), (basis, bas), (transfer, tra),
        (near, nea), (leaf_cpl, lcp), (parent_cpl, pcp),
    )):
        c = pltpu.make_async_copy(src, dst, in_sems.at[n])
        c.start()
        loads.append(c)

    barrier = pltpu.get_barrier_semaphore()
    for to in [place(*p) for p in PARTNERS] + [next_dev, prev_dev]:
        pl.semaphore_signal(barrier, inc=1, device_id=to, device_id_type=MESH)

    turned[...] = jnp.zeros((NDEV, NDEV), I32)
    turned[0:KP, 0:NP] = owner[...]
    turned[KP:2 * KP, 0:NP] = local[...]
    both_t = turned[...].T
    own = both_t[:NP, 0:KP]
    loc = both_t[:NP, KP:2 * KP]
    lane = lax.broadcasted_iota(I32, (NP, NDEV), 1)
    hits = jnp.zeros((NP, NDEV), I32)
    wanted = jnp.zeros((NP, NDEV), I32)
    for k in range(KP):
        eq = own[:, k:k + 1] == lane
        hits += jnp.where(eq, 1, 0)
        wanted += jnp.where(eq, loc[:, k:k + 1], 0)
    seen = jnp.zeros((1, NDEV), I32)
    rows = [jnp.zeros((1, NDEV), I32) for _ in range(CAP)]
    for p in range(NP):
        ranks[p:p + 1, :] = seen
        hit = hits[p:p + 1, :]
        for q in range(CAP):
            rows[q] = jnp.where((hit > 0) & (seen == q), wanted[p:p + 1, :], rows[q])
        seen = seen + hit
    for q in range(CAP):
        ask[q:q + 1, :] = rows[q]
        asked[len(PARTNERS), q:q + 1, :] = rows[q]

    for c in loads[:3]:
        c.wait()
    low32 = lax.broadcasted_iota(I32, (32, 128), 1) < 64
    low8 = lax.broadcasted_iota(I32, (8, 128), 1) < 64
    low4 = lax.broadcasted_iota(I32, (4, 128), 1) < 64

    def up_leaf(i, _):
        for u in range(8):
            p = i * 8 + u
            a = pts[pl.ds(2 + 2 * p, 2)].reshape(64, 128)
            b = bas[pl.ds(2 * p, 2)].reshape(128, 128)
            both = dot_last(a, b)
            pair = jnp.where(low32, both[:32], both[32:])
            swap = pltpu.roll(pair, 64, 1)
            pair_buf[p] = pair.astype(BF16)
            coef[5 + 2 * p] = jnp.where(low32, pair, swap).astype(BF16)
            coef[6 + 2 * p] = jnp.where(low32, swap, pair).astype(BF16)
        return 0

    lax.fori_loop(0, NP // 8, up_leaf, 0)
    block = [at[r[1]] * 4 + at[r[0]] for r in ROUTES]

    def up_parent(i, _):
        for u in range(8):
            p = i * 8 + u
            t = tra[p]
            twice = dot_last(pair_buf[p], jnp.concatenate([t, t], axis=0))
            for q in range(NQ):
                v = twice[8 * q:8 * q + 8]
                held[q][block[q], p] = jnp.where(low8, v, pltpu.roll(v, 4, 0))[:4].astype(BF16)
        return 0

    lax.fori_loop(0, NP // 8, up_parent, 0)

    pl.semaphore_wait(barrier, len(PARTNERS) + 2)

    def pass_on(q, src, axis, d, sem):
        pltpu.make_async_remote_copy(
            src_ref=held[q].at[src], dst_ref=held[q].at[src], send_sem=held_send.at[q],
            recv_sem=sem.at[q],
            device_id=place(axis, d, 0), device_id_type=MESH,
        ).start()

    for q, r in enumerate(ROUTES):
        for d in (1, 3, 2):
            pass_on(q, block[q], r[0], d, first_recv)
    for n, p in enumerate(PARTNERS):
        back = [i for i, o in enumerate(PARTNERS) if o == (p[0], (4 - p[1]) % 4, p[2])][0]
        pltpu.make_async_remote_copy(
            src_ref=ask, dst_ref=asked.at[back], send_sem=ask_send, recv_sem=ask_recv,
            device_id=place(*p), device_id_type=MESH,
        ).start()
    halos = []
    for n, (src, dst, dev) in enumerate((
        (pts.at[pl.ds(64, 2)], pts.at[pl.ds(0, 2)], next_dev),
        (pts.at[pl.ds(2, 2)], pts.at[pl.ds(66, 2)], prev_dev),
        (coef.at[pl.ds(64, 5)], coef.at[pl.ds(0, 5)], next_dev),
        (coef.at[pl.ds(5, 5)], coef.at[pl.ds(69, 5)], prev_dev),
    )):
        h = pltpu.make_async_remote_copy(
            src_ref=src, dst_ref=dst, send_sem=halo_send.at[n], recv_sem=halo_recv.at[n],
            device_id=dev, device_id_type=MESH,
        )
        h.start()
        halos.append(h)
    for q, r in enumerate(ROUTES):
        for d in (1, 3, 2):
            pass_on(q, block[q], r[1], d, second_recv)

    before = ranks[...]
    coords = (own // 32, rem(own // 2, 4), rem(own // 16, 2) * 2 + rem(own, 2))
    own_core = rem(own // 8, 2)
    slot = jnp.zeros((NP, NDEV), I32)
    for k in range(KP):
        eq = own[:, k:k + 1] == lane
        rank = jnp.sum(jnp.where(eq, before, 0), axis=1, keepdims=True)
        for n, r in enumerate(ROUTES):
            value = (coords[r[2]] * 2 + own_core) * 64 + (coords[r[1]] * 4 + coords[r[0]]) * 4
            slot = jnp.where(lane == n * KP + k, value[:, k:k + 1] + rank, slot)
    slots_v[...] = slot
    slot_copy = pltpu.make_async_copy(slots_v, slots_s, slot_sem)
    slot_copy.start()

    def wait_part(part, sem):
        pltpu.make_async_copy(part, part, sem).wait()

    for q, r in enumerate(ROUTES):
        wait_part(held[q].at[pl.ds(0, 3)], first_recv.at[q])
        for e in (1, 3, 2):
            src = at[r[1]] * 4 + rem(at[r[0]] + e, 4)
            for d in (1, 3, 2):
                pass_on(q, src, r[1], d, second_recv)

    wait_part(asked.at[pl.ds(0, len(PARTNERS))], ask_recv)
    asked_copy = pltpu.make_async_copy(asked, asked_s, asked_sem)
    asked_copy.start()

    for h in halos:
        h.wait()

    @pl.when(me == 0)
    def _():
        pts[0:2] = jnp.zeros((2, 32, 128), BF16)
        coef[0:5] = jnp.zeros((5, 32, 128), BF16)

    @pl.when(me == NDEV - 1)
    def _():
        pts[66:68] = jnp.zeros((2, 32, 128), BF16)
        coef[69:74] = jnp.zeros((5, 32, 128), BF16)

    loads[4].wait()

    def leaf_body(i, _):
        for u in range(8):
            p = i * 8 + u
            w = lcp[pl.ds(2 * p, 2)].reshape(128, 256)
            sides = []
            for j in range(2):
                c = 2 * p + j
                src = [coef[c + 5 + cpl_off[k, c]] for k in range(4)]
                sides.append(jnp.concatenate(
                    [jnp.where(low32, src[0], src[1]), jnp.where(low32, src[2], src[3])], axis=1
                ))
            both = dot_last(jnp.concatenate(sides, axis=0), w)
            leaf_acc[p] = jnp.where(low32, both[:32], both[32:])
        return 0

    lax.fori_loop(0, NP // 8, leaf_body, 0)
    loads[5].wait()
    asked_copy.wait()
    slot_copy.wait()

    base = core * 8
    for q, r in enumerate(ROUTES):
        wait_part(held[q].at[pl.ds(0, 12)], second_recv.at[q])
        fixed = adds[r[2]](at[r[2]])
        fixed = base + fixed[0] * 8 + fixed[1]

        def gather(ref, offset, n):
            def some(i, _):
                add2 = adds[r[1]](i)
                for j in range(4):
                    add1 = adds[r[0]](jnp.int32(j))
                    who = fixed + (add1[0] + add2[0]) * 8 + add1[1] + add2[1]
                    for c in range(CAP):
                        ref[offset + (i * 4 + j) * CAP + c] = held[q][
                            i * 4 + j, asked_s[n, c, who]
                        ]
                return 0

            lax.fori_loop(0, 4, some, 0)

        mine = (at[r[2]] * 2 + core) * 64
        line = [(i, p) for i, p in enumerate(PARTNERS) if p[0] == r[2] and p[1]]
        line.append((len(PARTNERS) - 1, PARTNERS[-1]))
        for m, (n, p) in enumerate(line):
            start = (q * 7 + m) * 64
            gather(send_buf, start, n)
            pltpu.make_async_remote_copy(
                src_ref=send_buf.at[pl.ds(start, 64)], dst_ref=recv_buf[q].at[pl.ds(mine, 64)],
                send_sem=data_send, recv_sem=data_recv.at[q],
                device_id=place(r[2], p[1], p[2]), device_id_type=MESH,
            ).start()
        gather(recv_buf[q], mine, len(PARTNERS))

    loads[3].wait()

    def near_body(i, _):
        for u in range(8):
            c = i * 8 + u
            acc = None
            for k in range(3):
                term = dot_last(pts[c + 2 + near_off[k, c]], nea[c, k])
                acc = term if acc is None else acc + term
            near_acc[c] = acc
        return 0

    lax.fori_loop(0, NL // 8, near_body, 0)
    for q in range(NQ):
        wait_part(recv_buf[q].at[pl.ds(0, 448)], data_recv.at[q])

        def stage(i, _):
            for u in range(8):
                p = i * 8 + u
                for m in range(KP // 2):
                    k = q * KP + 2 * m
                    va = recv_buf[q][slots_s[p, k]]
                    vb = recv_buf[q][slots_s[p, k + 1]]
                    cols = slice(m * 128, (m + 1) * 128)
                    staged[p, 8 * q:8 * q + 4, cols] = jnp.where(low4, va, pltpu.roll(vb, 64, 1))
                    staged[p, 8 * q + 4:8 * q + 8, cols] = jnp.where(low4, pltpu.roll(va, 64, 1), vb)
            return 0

        lax.fori_loop(0, NP // 8, stage, 0)

    def down(i, _):
        ps = [i * 16 + u for u in range(16)]
        halves = [dot_last(staged[p], pcp[p]).astype(BF16) for p in ps]
        downs = [dot(h, tra[p]) for h, p in zip(halves, ps)]
        for p, d in zip(ps, downs):
            total = leaf_acc[p] + d
            zero = jnp.zeros_like(total)
            both = jnp.concatenate(
                [jnp.where(low32, total, zero), jnp.where(low32, zero, total)], axis=0
            ).astype(BF16)
            far = dot(both, bas[pl.ds(2 * p, 2)].reshape(128, 128))
            res = far + near_acc[pl.ds(2 * p, 2)].reshape(64, 128)
            out[pl.ds(2 * p, 2)] = res.astype(BF16).reshape(2, 32, 128)
        return 0

    lax.fori_loop(0, NP // 16, down, 0)
    wait_part(send_buf, data_send)
    for q in range(NQ):
        wait_part(held[q].at[pl.ds(0, 15)], held_send.at[q])
    wait_part(asked.at[pl.ds(0, len(PARTNERS))], ask_send)


def on_device(*args):
    anywhere = pl.BlockSpec(memory_space=pl.ANY)
    smem = pl.BlockSpec(memory_space=pltpu.SMEM)
    vmem = pl.BlockSpec(memory_space=pltpu.VMEM)
    dma = pltpu.SemaphoreType.DMA
    return pl.pallas_call(
        kernel,
        out_shape=jax.ShapeDtypeStruct((NL, 32, 128), BF16),
        in_specs=[anywhere]*6 + [smem] * 2 + [vmem] * 2,
        out_specs=vmem,
        scratch_shapes=[
            pltpu.VMEM((NL + 4, 32, 128), BF16),
            pltpu.VMEM((NL, 64, 128), BF16),
            pltpu.VMEM((NP, 64, 128), BF16),
            pltpu.VMEM((NL, 64, 256), BF16),
            pltpu.VMEM((NP, 64, 512), BF16),
            pltpu.VMEM((NL, 3, 128, 128), BF16),
            pltpu.VMEM((NL + 10, 32, 128), BF16),
            pltpu.VMEM((NP, 32, 128), BF16),
            pltpu.VMEM((NL, 32, 128), F32),
            pltpu.VMEM((NP, 32, 128), F32),
            pltpu.VMEM((NP, 32, 512), BF16),
            pltpu.VMEM((NDEV, NDEV), I32),
            pltpu.VMEM((CAP, NDEV), I32),
            pltpu.VMEM((len(PARTNERS) + 1, CAP, NDEV), I32),
            pltpu.VMEM((NP, NDEV), I32),
            pltpu.VMEM((NP, NDEV), I32),
            pltpu.VMEM((NQ * 7 * 64, 4, 128), BF16),
            pltpu.VMEM((NL, 32, 128), BF16),
            pltpu.SMEM((len(PARTNERS) + 1, CAP, NDEV), I32),
            pltpu.SMEM((NP, NDEV), I32),
            dma((6,)), dma, dma, dma, dma, dma, dma((4,)), dma((4,)),
            dma((NQ,)), dma((NQ,)), dma((NQ,)), dma, dma((NQ,)),
            *[pltpu.VMEM((16, NP, 4, 128), BF16)] * NQ,
            *[pltpu.VMEM((512, 4, 128), BF16)] * NQ,
        ],
        compiler_params=pltpu.CompilerParams(
            collective_id=0, has_side_effects=True, vmem_limit_bytes=48 * 1024 * 1024
        ),
        name="h2",
    )(*[pltpu.with_memory_space_constraint(a, pltpu.HBM) for a in args[:6] + tuple(v.T for v in args[6:])])


def solution(mesh):
    both = ("stream", "leaf")
    placed = tuple(P(both, *([None] * n)) for n in (2, 2, 2, 2, 2, 3, 1, 1, 1, 1))
    return jax.shard_map(
        on_device, mesh=mesh, in_specs=placed, out_specs=P(both, None, None), check_vma=False
    )
```

```python
import jax
import jax.numpy as jnp
from jax import lax
from jax.experimental import pallas as pl
from jax.experimental.pallas import tpu as pltpu
from jax.sharding import PartitionSpec as P

MESH = pl.DeviceIdType.MESH
F32 = jnp.float32
BF16 = jnp.bfloat16
I32 = jnp.int32
NDEV = 128
NL = 64
NP = 32
KP = 8
CAP = 4
LAST = (((1,), (1,)), ((), ()))


NQ = 4
ROUTES = ((0, 1, 2), (1, 2, 0), (2, 0, 1), (0, 1, 2))
PARTNERS = [(a, d, dc) for a in range(3) for d in (2, 1, 3) for dc in range(2)] + [(0, 0, 1)]


def dot_last(a, b):
    return lax.dot_general(a, b, LAST, preferred_element_type=F32)


def dot(a, b):
    return jnp.dot(a, b, preferred_element_type=F32)


def kernel(*refs):
    held, recv_buf = refs[-8:-4], refs[-4:]
    body(*refs[:-8], held, recv_buf)


def body(
    points, basis, transfer, leaf_cpl, parent_cpl, near, near_off, cpl_off, owner, local, out,
    pts, bas, tra, lcp, pcp, nea,
    coef, pair_buf, near_acc, leaf_acc, staged,
    turned, ask, asked, slots_v, ranks,
    send_buf, out_buf,
    asked_s, slots_s,
    in_sems, slot_sem, asked_sem, out_sem, ask_send, ask_recv, halo_send, halo_recv,
    held_send, first_recv, second_recv, data_send, data_recv,
    held, recv_buf,
):
    s = lax.axis_index("stream")
    l = lax.axis_index("leaf")
    rem = lambda a, b: lax.rem(a, jnp.int32(b))
    div = lambda a, b: lax.div(a, jnp.int32(b))
    core = rem(s, 2)
    at = (div(s, 4), div(l, 2), rem(div(s, 2), 2) * 2 + rem(l, 2))
    me = s * 8 + l

    adds = (
        lambda v: (v * 4, 0),
        lambda v: (0, v * 2),
        lambda v: (div(v, 2) * 2, rem(v, 2)),
    )
    shifted = [[adds[a](rem(at[a] + d, 4)) for d in range(4)] for a in range(3)]

    def place(a, d, dc):
        st = core if dc == 0 else 1 - core
        lf = 0
        for axis in range(3):
            part = shifted[axis][d if axis == a else 0]
            st = st + part[0]
            lf = lf + part[1]
        return st, lf

    following = rem(me + 1, NDEV)
    previous = rem(me + NDEV - 1, NDEV)
    next_dev = (div(following, 8), rem(following, 8))
    prev_dev = (div(previous, 8), rem(previous, 8))

    loads = []
    for n, (src, dst) in enumerate((
        (points, pts.at[pl.ds(2, NL)]), (basis, bas), (transfer, tra),
        (near, nea), (leaf_cpl, lcp), (parent_cpl, pcp),
    )):
        c = pltpu.make_async_copy(src, dst, in_sems.at[n])
        c.start()
        loads.append(c)

    barrier = pltpu.get_barrier_semaphore()
    for to in [place(*p) for p in PARTNERS] + [next_dev, prev_dev]:
        pl.semaphore_signal(barrier, inc=1, device_id=to, device_id_type=MESH)

    turned[...] = jnp.zeros((NDEV, NDEV), I32)
    turned[0:KP, 0:NP] = owner[...]
    turned[KP:2 * KP, 0:NP] = local[...]
    both_t = turned[...].T
    own = both_t[:NP, 0:KP]
    loc = both_t[:NP, KP:2 * KP]
    lane = lax.broadcasted_iota(I32, (NP, NDEV), 1)
    hits = jnp.zeros((NP, NDEV), I32)
    wanted = jnp.zeros((NP, NDEV), I32)
    for k in range(KP):
        eq = own[:, k:k + 1] == lane
        hits += jnp.where(eq, 1, 0)
        wanted += jnp.where(eq, loc[:, k:k + 1], 0)
    seen = jnp.zeros((1, NDEV), I32)
    rows = [jnp.zeros((1, NDEV), I32) for _ in range(CAP)]
    for p in range(NP):
        ranks[p:p + 1, :] = seen
        hit = hits[p:p + 1, :]
        for q in range(CAP):
            rows[q] = jnp.where((hit > 0) & (seen == q), wanted[p:p + 1, :], rows[q])
        seen = seen + hit
    for q in range(CAP):
        ask[q:q + 1, :] = rows[q]
        asked[len(PARTNERS), q:q + 1, :] = rows[q]

    for c in loads[:3]:
        c.wait()
    low32 = lax.broadcasted_iota(I32, (32, 128), 1) < 64
    low8 = lax.broadcasted_iota(I32, (8, 128), 1) < 64
    low4 = lax.broadcasted_iota(I32, (4, 128), 1) < 64

    def up_leaf(i, _):
        for u in range(8):
            p = i * 8 + u
            a = pts[pl.ds(2 + 2 * p, 2)].reshape(64, 128)
            b = bas[pl.ds(2 * p, 2)].reshape(128, 128)
            both = dot_last(a, b)
            pair = jnp.where(low32, both[:32], both[32:])
            swap = pltpu.roll(pair, 64, 1)
            pair_buf[p] = pair.astype(BF16)
            coef[5 + 2 * p] = jnp.where(low32, pair, swap).astype(BF16)
            coef[6 + 2 * p] = jnp.where(low32, swap, pair).astype(BF16)
        return 0

    lax.fori_loop(0, NP // 8, up_leaf, 0)
    block = [at[r[1]] * 4 + at[r[0]] for r in ROUTES]

    def up_parent(i, _):
        for u in range(8):
            p = i * 8 + u
            t = tra[p]
            twice = dot_last(pair_buf[p], jnp.concatenate([t, t], axis=0))
            for q in range(NQ):
                v = twice[8 * q:8 * q + 8]
                held[q][block[q], p] = jnp.where(low8, v, pltpu.roll(v, 4, 0))[:4].astype(BF16)
        return 0

    lax.fori_loop(0, NP // 8, up_parent, 0)

    pl.semaphore_wait(barrier, len(PARTNERS) + 2)

    def pass_on(q, src, half, axis, d, sem):
        part = held[q].at[src, pl.ds(half * (NP // 2), NP // 2)]
        pltpu.make_async_remote_copy(
            src_ref=part, dst_ref=part, send_sem=held_send.at[q],
            recv_sem=sem.at[q],
            device_id=place(axis, d, 0), device_id_type=MESH,
        ).start()

    for q, r in enumerate(ROUTES):
        for d in (1, 3, 2):
            for half in range(2):
                pass_on(q, block[q], half, r[half], d, first_recv)
    for n, p in enumerate(PARTNERS):
        back = [i for i, o in enumerate(PARTNERS) if o == (p[0], (4 - p[1]) % 4, p[2])][0]
        pltpu.make_async_remote_copy(
            src_ref=ask, dst_ref=asked.at[back], send_sem=ask_send, recv_sem=ask_recv,
            device_id=place(*p), device_id_type=MESH,
        ).start()
    halos = []
    for n, (src, dst, dev) in enumerate((
        (pts.at[pl.ds(64, 2)], pts.at[pl.ds(0, 2)], next_dev),
        (pts.at[pl.ds(2, 2)], pts.at[pl.ds(66, 2)], prev_dev),
        (coef.at[pl.ds(64, 5)], coef.at[pl.ds(0, 5)], next_dev),
        (coef.at[pl.ds(5, 5)], coef.at[pl.ds(69, 5)], prev_dev),
    )):
        h = pltpu.make_async_remote_copy(
            src_ref=src, dst_ref=dst, send_sem=halo_send.at[n], recv_sem=halo_recv.at[n],
            device_id=dev, device_id_type=MESH,
        )
        h.start()
        halos.append(h)
    for q, r in enumerate(ROUTES):
        for d in (1, 3, 2):
            for half in range(2):
                pass_on(q, block[q], half, r[1 - half], d, second_recv)

    before = ranks[...]
    coords = (own // 32, rem(own // 2, 4), rem(own // 16, 2) * 2 + rem(own, 2))
    own_core = rem(own // 8, 2)
    slot = jnp.zeros((NP, NDEV), I32)
    for k in range(KP):
        eq = own[:, k:k + 1] == lane
        rank = jnp.sum(jnp.where(eq, before, 0), axis=1, keepdims=True)
        for n, r in enumerate(ROUTES):
            value = (coords[r[2]] * 2 + own_core) * 64 + (coords[r[1]] * 4 + coords[r[0]]) * 4
            slot = jnp.where(lane == n * KP + k, value[:, k:k + 1] + rank, slot)
    slots_v[...] = slot
    slot_copy = pltpu.make_async_copy(slots_v, slots_s, slot_sem)
    slot_copy.start()

    def wait_part(part, sem):
        pltpu.make_async_copy(part, part, sem).wait()

    for q, r in enumerate(ROUTES):
        wait_part(held[q].at[pl.ds(0, 3)], first_recv.at[q])
        for e in (1, 3, 2):
            src = (
                at[r[1]] * 4 + rem(at[r[0]] + e, 4),
                rem(at[r[1]] + e, 4) * 4 + at[r[0]],
            )
            for d in (1, 3, 2):
                for half in range(2):
                    pass_on(q, src[half], half, r[1 - half], d, second_recv)

    wait_part(asked.at[pl.ds(0, len(PARTNERS))], ask_recv)
    asked_copy = pltpu.make_async_copy(asked, asked_s, asked_sem)
    asked_copy.start()

    for h in halos:
        h.wait()

    @pl.when(me == 0)
    def _():
        pts[0:2] = jnp.zeros((2, 32, 128), BF16)
        coef[0:5] = jnp.zeros((5, 32, 128), BF16)

    @pl.when(me == NDEV - 1)
    def _():
        pts[66:68] = jnp.zeros((2, 32, 128), BF16)
        coef[69:74] = jnp.zeros((5, 32, 128), BF16)

    loads[4].wait()

    def leaf_body(i, _):
        for u in range(8):
            p = i * 8 + u
            w = lcp[pl.ds(2 * p, 2)].reshape(128, 256)
            sides = []
            for j in range(2):
                c = 2 * p + j
                src = [coef[c + 5 + cpl_off[k, c]] for k in range(4)]
                sides.append(jnp.concatenate(
                    [jnp.where(low32, src[0], src[1]), jnp.where(low32, src[2], src[3])], axis=1
                ))
            both = dot_last(jnp.concatenate(sides, axis=0), w)
            leaf_acc[p] = jnp.where(low32, both[:32], both[32:])
        return 0

    lax.fori_loop(0, NP // 8, leaf_body, 0)
    loads[5].wait()
    asked_copy.wait()
    slot_copy.wait()

    base = core * 8
    for q, r in enumerate(ROUTES):
        wait_part(held[q].at[pl.ds(0, 12)], second_recv.at[q])
        fixed = adds[r[2]](at[r[2]])
        fixed = base + fixed[0] * 8 + fixed[1]

        def gather(ref, offset, n):
            def some(i, _):
                add2 = adds[r[1]](i)
                for j in range(4):
                    add1 = adds[r[0]](jnp.int32(j))
                    who = fixed + (add1[0] + add2[0]) * 8 + add1[1] + add2[1]
                    for c in range(CAP):
                        ref[offset + (i * 4 + j) * CAP + c] = held[q][
                            i * 4 + j, asked_s[n, c, who]
                        ]
                return 0

            lax.fori_loop(0, 4, some, 0)

        mine = (at[r[2]] * 2 + core) * 64
        line = [(i, p) for i, p in enumerate(PARTNERS) if p[0] == r[2] and p[1]]
        line.append((len(PARTNERS) - 1, PARTNERS[-1]))
        for m, (n, p) in enumerate(line):
            start = (q * 7 + m) * 64
            gather(send_buf, start, n)
            pltpu.make_async_remote_copy(
                src_ref=send_buf.at[pl.ds(start, 64)], dst_ref=recv_buf[q].at[pl.ds(mine, 64)],
                send_sem=data_send, recv_sem=data_recv.at[q],
                device_id=place(r[2], p[1], p[2]), device_id_type=MESH,
            ).start()
        gather(recv_buf[q], mine, len(PARTNERS))

    loads[3].wait()

    def near_body(i, _):
        for u in range(8):
            c = i * 8 + u
            acc = None
            for k in range(3):
                term = dot_last(pts[c + 2 + near_off[k, c]], nea[c, k])
                acc = term if acc is None else acc + term
            near_acc[c] = acc
        return 0

    lax.fori_loop(0, NL // 8, near_body, 0)
    for q in range(NQ):
        wait_part(recv_buf[q].at[pl.ds(0, 448)], data_recv.at[q])

        def stage(i, _):
            for u in range(8):
                p = i * 8 + u
                for m in range(KP // 2):
                    k = q * KP + 2 * m
                    va = recv_buf[q][slots_s[p, k]]
                    vb = recv_buf[q][slots_s[p, k + 1]]
                    cols = slice(m * 128, (m + 1) * 128)
                    staged[p, 8 * q:8 * q + 4, cols] = jnp.where(low4, va, pltpu.roll(vb, 64, 1))
                    staged[p, 8 * q + 4:8 * q + 8, cols] = jnp.where(low4, pltpu.roll(va, 64, 1), vb)
            return 0

        lax.fori_loop(0, NP // 8, stage, 0)

    def down(i, _):
        ps = [i * 16 + u for u in range(16)]
        halves = [dot_last(staged[p], pcp[p]).astype(BF16) for p in ps]
        downs = [dot(h, tra[p]) for h, p in zip(halves, ps)]
        for p, d in zip(ps, downs):
            total = leaf_acc[p] + d
            zero = jnp.zeros_like(total)
            both = jnp.concatenate(
                [jnp.where(low32, total, zero), jnp.where(low32, zero, total)], axis=0
            ).astype(BF16)
            far = dot(both, bas[pl.ds(2 * p, 2)].reshape(128, 128))
            res = far + near_acc[pl.ds(2 * p, 2)].reshape(64, 128)
            out[pl.ds(2 * p, 2)] = res.astype(BF16).reshape(2, 32, 128)
        return 0

    lax.fori_loop(0, NP // 16, down, 0)
    wait_part(send_buf, data_send)
    for q in range(NQ):
        wait_part(held[q].at[pl.ds(0, 15)], held_send.at[q])
    wait_part(asked.at[pl.ds(0, len(PARTNERS))], ask_send)


def on_device(*args):
    anywhere = pl.BlockSpec(memory_space=pl.ANY)
    smem = pl.BlockSpec(memory_space=pltpu.SMEM)
    vmem = pl.BlockSpec(memory_space=pltpu.VMEM)
    dma = pltpu.SemaphoreType.DMA
    return pl.pallas_call(
        kernel,
        out_shape=jax.ShapeDtypeStruct((NL, 32, 128), BF16),
        in_specs=[anywhere]*6 + [smem] * 2 + [vmem] * 2,
        out_specs=vmem,
        scratch_shapes=[
            pltpu.VMEM((NL + 4, 32, 128), BF16),
            pltpu.VMEM((NL, 64, 128), BF16),
            pltpu.VMEM((NP, 64, 128), BF16),
            pltpu.VMEM((NL, 64, 256), BF16),
            pltpu.VMEM((NP, 64, 512), BF16),
            pltpu.VMEM((NL, 3, 128, 128), BF16),
            pltpu.VMEM((NL + 10, 32, 128), BF16),
            pltpu.VMEM((NP, 32, 128), BF16),
            pltpu.VMEM((NL, 32, 128), F32),
            pltpu.VMEM((NP, 32, 128), F32),
            pltpu.VMEM((NP, 32, 512), BF16),
            pltpu.VMEM((NDEV, NDEV), I32),
            pltpu.VMEM((CAP, NDEV), I32),
            pltpu.VMEM((len(PARTNERS) + 1, CAP, NDEV), I32),
            pltpu.VMEM((NP, NDEV), I32),
            pltpu.VMEM((NP, NDEV), I32),
            pltpu.VMEM((NQ * 7 * 64, 4, 128), BF16),
            pltpu.VMEM((NL, 32, 128), BF16),
            pltpu.SMEM((len(PARTNERS) + 1, CAP, NDEV), I32),
            pltpu.SMEM((NP, NDEV), I32),
            dma((6,)), dma, dma, dma, dma, dma, dma((4,)), dma((4,)),
            dma((NQ,)), dma((NQ,)), dma((NQ,)), dma, dma((NQ,)),
            *[pltpu.VMEM((16, NP, 4, 128), BF16)] * NQ,
            *[pltpu.VMEM((512, 4, 128), BF16)] * NQ,
        ],
        compiler_params=pltpu.CompilerParams(
            collective_id=0, has_side_effects=True, vmem_limit_bytes=48 * 1024 * 1024
        ),
        name="h2",
    )(*[pltpu.with_memory_space_constraint(a, pltpu.HBM) for a in args[:6] + tuple(v.T for v in args[6:])])


def solution(mesh):
    both = ("stream", "leaf")
    placed = tuple(P(both, *([None] * n)) for n in (2, 2, 2, 2, 2, 3, 1, 1, 1, 1))
    return jax.shard_map(
        on_device, mesh=mesh, in_specs=placed, out_specs=P(both, None, None), check_vma=False
    )
```

```python
import jax
import jax.numpy as jnp
from jax import lax
from jax.experimental import pallas as pl
from jax.experimental.pallas import tpu as pltpu
from jax.sharding import PartitionSpec as P

MESH = pl.DeviceIdType.MESH
F32 = jnp.float32
BF16 = jnp.bfloat16
I32 = jnp.int32
NDEV = 128
NL = 64
NP = 32
KP = 8
CAP = 4
LAST = (((1,), (1,)), ((), ()))


NQ = 4
ROUTES = ((0, 1, 2), (1, 2, 0), (2, 0, 1), (0, 1, 2))
PARTNERS = [(a, d, dc) for a in range(3) for d in (2, 1, 3) for dc in range(2)] + [(0, 0, 1)]


def dot_last(a, b):
    return lax.dot_general(a, b, LAST, preferred_element_type=F32)


def dot(a, b):
    return jnp.dot(a, b, preferred_element_type=F32)


def kernel(*refs):
    held, recv_buf = refs[-8:-4], refs[-4:]
    body(*refs[:-8], held, recv_buf)


def body(
    points, basis, transfer, leaf_cpl, parent_cpl, near, near_off, cpl_off, owner, local, out,
    pts, bas, tra, lcp, pcp, nea,
    coef, pair_buf, near_acc, leaf_acc, staged,
    turned, ask, asked, slots_v, ranks,
    send_buf, out_buf,
    asked_s, slots_s,
    in_sems, slot_sem, asked_sem, out_sem, ask_send, ask_recv, halo_send, halo_recv,
    held_send, first_recv, second_recv, data_send, data_recv,
    held, recv_buf,
):
    s = lax.axis_index("stream")
    l = lax.axis_index("leaf")
    rem = lambda a, b: lax.rem(a, jnp.int32(b))
    div = lambda a, b: lax.div(a, jnp.int32(b))
    core = rem(s, 2)
    at = (div(s, 4), div(l, 2), rem(div(s, 2), 2) * 2 + rem(l, 2))
    me = s * 8 + l

    adds = (
        lambda v: (v * 4, 0),
        lambda v: (0, v * 2),
        lambda v: (div(v, 2) * 2, rem(v, 2)),
    )
    shifted = [[adds[a](rem(at[a] + d, 4)) for d in range(4)] for a in range(3)]

    def place(a, d, dc):
        st = core if dc == 0 else 1 - core
        lf = 0
        for axis in range(3):
            part = shifted[axis][d if axis == a else 0]
            st = st + part[0]
            lf = lf + part[1]
        return st, lf

    following = rem(me + 1, NDEV)
    previous = rem(me + NDEV - 1, NDEV)
    next_dev = (div(following, 8), rem(following, 8))
    prev_dev = (div(previous, 8), rem(previous, 8))

    loads = []
    for n, (src, dst) in enumerate((
        (points, pts.at[pl.ds(2, NL)]), (basis, bas), (transfer, tra),
        (near, nea), (leaf_cpl, lcp), (parent_cpl, pcp),
    )):
        c = pltpu.make_async_copy(src, dst, in_sems.at[n])
        c.start()
        loads.append(c)

    barrier = pltpu.get_barrier_semaphore()
    for to in [place(*p) for p in PARTNERS] + [next_dev, prev_dev]:
        pl.semaphore_signal(barrier, inc=1, device_id=to, device_id_type=MESH)

    turned[...] = jnp.zeros((NDEV, NDEV), I32)
    turned[0:KP, 0:NP] = owner[...]
    turned[KP:2 * KP, 0:NP] = local[...]
    both_t = turned[...].T
    own = both_t[:NP, 0:KP]
    loc = both_t[:NP, KP:2 * KP]
    lane = lax.broadcasted_iota(I32, (NP, NDEV), 1)
    hits = jnp.zeros((NP, NDEV), I32)
    wanted = jnp.zeros((NP, NDEV), I32)
    for k in range(KP):
        eq = own[:, k:k + 1] == lane
        hits += jnp.where(eq, 1, 0)
        wanted += jnp.where(eq, loc[:, k:k + 1], 0)
    seen = jnp.zeros((1, NDEV), I32)
    rows = [jnp.zeros((1, NDEV), I32) for _ in range(CAP)]
    for p in range(NP):
        ranks[p:p + 1, :] = seen
        hit = hits[p:p + 1, :]
        for q in range(CAP):
            rows[q] = jnp.where((hit > 0) & (seen == q), wanted[p:p + 1, :], rows[q])
        seen = seen + hit
    for q in range(CAP):
        ask[q:q + 1, :] = rows[q]
        asked[len(PARTNERS), q:q + 1, :] = rows[q]

    for c in loads[:3]:
        c.wait()
    low32 = lax.broadcasted_iota(I32, (32, 128), 1) < 64
    low8 = lax.broadcasted_iota(I32, (8, 128), 1) < 64
    low4 = lax.broadcasted_iota(I32, (4, 128), 1) < 64

    def up_leaf(i, _):
        for u in range(8):
            p = i * 8 + u
            a = pts[pl.ds(2 + 2 * p, 2)].reshape(64, 128)
            b = bas[pl.ds(2 * p, 2)].reshape(128, 128)
            both = dot_last(a, b)
            pair = jnp.where(low32, both[:32], both[32:])
            swap = pltpu.roll(pair, 64, 1)
            pair_buf[p] = pair.astype(BF16)
            coef[5 + 2 * p] = jnp.where(low32, pair, swap).astype(BF16)
            coef[6 + 2 * p] = jnp.where(low32, swap, pair).astype(BF16)
        return 0

    lax.fori_loop(0, NP // 8, up_leaf, 0)
    block = [at[r[1]] * 4 + at[r[0]] for r in ROUTES]

    def up_parent(i, _):
        for u in range(8):
            p = i * 8 + u
            t = tra[p]
            twice = dot_last(pair_buf[p], jnp.concatenate([t, t], axis=0))
            for q in range(NQ):
                v = twice[8 * q:8 * q + 8]
                held[q][block[q], p] = jnp.where(low8, v, pltpu.roll(v, 4, 0))[:4].astype(BF16)
        return 0

    lax.fori_loop(0, NP // 8, up_parent, 0)

    pl.semaphore_wait(barrier, len(PARTNERS) + 2)

    def pass_on(q, src, half, axis, d, sem):
        part = held[q].at[src, pl.ds(half * (NP // 2), NP // 2)]
        pltpu.make_async_remote_copy(
            src_ref=part, dst_ref=part, send_sem=held_send.at[q],
            recv_sem=sem.at[q],
            device_id=place(axis, d, 0), device_id_type=MESH,
        ).start()

    for q, r in enumerate(ROUTES):
        for d in (1, 3, 2):
            for half in range(2):
                pass_on(q, block[q], half, r[half], d, first_recv)
    for n, p in enumerate(PARTNERS):
        back = [i for i, o in enumerate(PARTNERS) if o == (p[0], (4 - p[1]) % 4, p[2])][0]
        pltpu.make_async_remote_copy(
            src_ref=ask, dst_ref=asked.at[back], send_sem=ask_send, recv_sem=ask_recv,
            device_id=place(*p), device_id_type=MESH,
        ).start()
    halos = []
    for n, (src, dst, dev) in enumerate((
        (pts.at[pl.ds(64, 2)], pts.at[pl.ds(0, 2)], next_dev),
        (pts.at[pl.ds(2, 2)], pts.at[pl.ds(66, 2)], prev_dev),
        (coef.at[pl.ds(64, 5)], coef.at[pl.ds(0, 5)], next_dev),
        (coef.at[pl.ds(5, 5)], coef.at[pl.ds(69, 5)], prev_dev),
    )):
        h = pltpu.make_async_remote_copy(
            src_ref=src, dst_ref=dst, send_sem=halo_send.at[n], recv_sem=halo_recv.at[n],
            device_id=dev, device_id_type=MESH,
        )
        h.start()
        halos.append(h)
    for q, r in enumerate(ROUTES):
        for d in (1, 3, 2):
            for half in range(2):
                pass_on(q, block[q], half, r[1 - half], d, second_recv)

    before = ranks[...]
    coords = (own // 32, rem(own // 2, 4), rem(own // 16, 2) * 2 + rem(own, 2))
    own_core = rem(own // 8, 2)
    slot = jnp.zeros((NP, NDEV), I32)
    for k in range(KP):
        eq = own[:, k:k + 1] == lane
        rank = jnp.sum(jnp.where(eq, before, 0), axis=1, keepdims=True)
        for n, r in enumerate(ROUTES):
            value = (coords[r[2]] * 2 + own_core) * 64 + (coords[r[1]] * 4 + coords[r[0]]) * 4
            slot = jnp.where(lane == n * KP + k, value[:, k:k + 1] + rank, slot)
    slots_v[...] = slot
    slot_copy = pltpu.make_async_copy(slots_v, slots_s, slot_sem)
    slot_copy.start()

    def wait_part(part, sem):
        pltpu.make_async_copy(part, part, sem).wait()

    for q, r in enumerate(ROUTES):
        wait_part(held[q].at[pl.ds(0, 3)], first_recv.at[q])
        for e in (1, 3, 2):
            src = (
                at[r[1]] * 4 + rem(at[r[0]] + e, 4),
                rem(at[r[1]] + e, 4) * 4 + at[r[0]],
            )
            for d in (1, 3, 2):
                for half in range(2):
                    pass_on(q, src[half], half, r[1 - half], d, second_recv)

    wait_part(asked.at[pl.ds(0, len(PARTNERS))], ask_recv)
    asked_copy = pltpu.make_async_copy(asked, asked_s, asked_sem)
    asked_copy.start()

    for h in halos:
        h.wait()

    @pl.when(me == 0)
    def _():
        pts[0:2] = jnp.zeros((2, 32, 128), BF16)
        coef[0:5] = jnp.zeros((5, 32, 128), BF16)

    @pl.when(me == NDEV - 1)
    def _():
        pts[66:68] = jnp.zeros((2, 32, 128), BF16)
        coef[69:74] = jnp.zeros((5, 32, 128), BF16)

    loads[5].wait()
    asked_copy.wait()
    slot_copy.wait()

    base = core * 8
    for q, r in enumerate(ROUTES):
        wait_part(held[q].at[pl.ds(0, 12)], second_recv.at[q])
        fixed = adds[r[2]](at[r[2]])
        fixed = base + fixed[0] * 8 + fixed[1]

        def gather(ref, offset, n):
            def some(i, _):
                add2 = adds[r[1]](i)
                for j in range(4):
                    add1 = adds[r[0]](jnp.int32(j))
                    who = fixed + (add1[0] + add2[0]) * 8 + add1[1] + add2[1]
                    for c in range(CAP):
                        ref[offset + (i * 4 + j) * CAP + c] = held[q][
                            i * 4 + j, asked_s[n, c, who]
                        ]
                return 0

            lax.fori_loop(0, 4, some, 0)

        mine = (at[r[2]] * 2 + core) * 64
        line = [(i, p) for i, p in enumerate(PARTNERS) if p[0] == r[2] and p[1]]
        line.append((len(PARTNERS) - 1, PARTNERS[-1]))
        for m, (n, p) in enumerate(line):
            start = (q * 7 + m) * 64
            gather(send_buf, start, n)
            pltpu.make_async_remote_copy(
                src_ref=send_buf.at[pl.ds(start, 64)], dst_ref=recv_buf[q].at[pl.ds(mine, 64)],
                send_sem=data_send, recv_sem=data_recv.at[q],
                device_id=place(r[2], p[1], p[2]), device_id_type=MESH,
            ).start()
        gather(recv_buf[q], mine, len(PARTNERS))

    loads[4].wait()

    def leaf_body(i, _):
        for u in range(8):
            p = i * 8 + u
            w = lcp[pl.ds(2 * p, 2)].reshape(128, 256)
            sides = []
            for j in range(2):
                c = 2 * p + j
                src = [coef[c + 5 + cpl_off[k, c]] for k in range(4)]
                sides.append(jnp.concatenate(
                    [jnp.where(low32, src[0], src[1]), jnp.where(low32, src[2], src[3])], axis=1
                ))
            both = dot_last(jnp.concatenate(sides, axis=0), w)
            leaf_acc[p] = jnp.where(low32, both[:32], both[32:])
        return 0

    lax.fori_loop(0, NP // 8, leaf_body, 0)
    loads[3].wait()

    def near_body(i, _):
        for u in range(8):
            c = i * 8 + u
            acc = None
            for k in range(3):
                term = dot_last(pts[c + 2 + near_off[k, c]], nea[c, k])
                acc = term if acc is None else acc + term
            near_acc[c] = acc
        return 0

    lax.fori_loop(0, NL // 8, near_body, 0)
    for q in range(NQ):
        wait_part(recv_buf[q].at[pl.ds(0, 448)], data_recv.at[q])

        def stage(i, _):
            for u in range(8):
                p = i * 8 + u
                for m in range(KP // 2):
                    k = q * KP + 2 * m
                    va = recv_buf[q][slots_s[p, k]]
                    vb = recv_buf[q][slots_s[p, k + 1]]
                    cols = slice(m * 128, (m + 1) * 128)
                    staged[p, 8 * q:8 * q + 4, cols] = jnp.where(low4, va, pltpu.roll(vb, 64, 1))
                    staged[p, 8 * q + 4:8 * q + 8, cols] = jnp.where(low4, pltpu.roll(va, 64, 1), vb)
            return 0

        if q < NQ - 1:
            lax.fori_loop(0, NP // 8, stage, 0)

    def down(i, _):
        for h in range(2):
            stage(i * 2 + h, 0)
        ps = [i * 16 + u for u in range(16)]
        halves = [dot_last(staged[p], pcp[p]).astype(BF16) for p in ps]
        downs = [dot(h, tra[p]) for h, p in zip(halves, ps)]
        for p, d in zip(ps, downs):
            total = leaf_acc[p] + d
            zero = jnp.zeros_like(total)
            both = jnp.concatenate(
                [jnp.where(low32, total, zero), jnp.where(low32, zero, total)], axis=0
            ).astype(BF16)
            far = dot(both, bas[pl.ds(2 * p, 2)].reshape(128, 128))
            res = far + near_acc[pl.ds(2 * p, 2)].reshape(64, 128)
            out[pl.ds(2 * p, 2)] = res.astype(BF16).reshape(2, 32, 128)
        return 0

    lax.fori_loop(0, NP // 16, down, 0)
    wait_part(send_buf, data_send)
    for q in range(NQ):
        wait_part(held[q].at[pl.ds(0, 15)], held_send.at[q])
    wait_part(asked.at[pl.ds(0, len(PARTNERS))], ask_send)


def on_device(*args):
    anywhere = pl.BlockSpec(memory_space=pl.ANY)
    smem = pl.BlockSpec(memory_space=pltpu.SMEM)
    vmem = pl.BlockSpec(memory_space=pltpu.VMEM)
    dma = pltpu.SemaphoreType.DMA
    return pl.pallas_call(
        kernel,
        out_shape=jax.ShapeDtypeStruct((NL, 32, 128), BF16),
        in_specs=[anywhere]*6 + [smem] * 2 + [vmem] * 2,
        out_specs=vmem,
        scratch_shapes=[
            pltpu.VMEM((NL + 4, 32, 128), BF16),
            pltpu.VMEM((NL, 64, 128), BF16),
            pltpu.VMEM((NP, 64, 128), BF16),
            pltpu.VMEM((NL, 64, 256), BF16),
            pltpu.VMEM((NP, 64, 512), BF16),
            pltpu.VMEM((NL, 3, 128, 128), BF16),
            pltpu.VMEM((NL + 10, 32, 128), BF16),
            pltpu.VMEM((NP, 32, 128), BF16),
            pltpu.VMEM((NL, 32, 128), F32),
            pltpu.VMEM((NP, 32, 128), F32),
            pltpu.VMEM((NP, 32, 512), BF16),
            pltpu.VMEM((NDEV, NDEV), I32),
            pltpu.VMEM((CAP, NDEV), I32),
            pltpu.VMEM((len(PARTNERS) + 1, CAP, NDEV), I32),
            pltpu.VMEM((NP, NDEV), I32),
            pltpu.VMEM((NP, NDEV), I32),
            pltpu.VMEM((NQ * 7 * 64, 4, 128), BF16),
            pltpu.VMEM((NL, 32, 128), BF16),
            pltpu.SMEM((len(PARTNERS) + 1, CAP, NDEV), I32),
            pltpu.SMEM((NP, NDEV), I32),
            dma((6,)), dma, dma, dma, dma, dma, dma((4,)), dma((4,)),
            dma((NQ,)), dma((NQ,)), dma((NQ,)), dma, dma((NQ,)),
            *[pltpu.VMEM((16, NP, 4, 128), BF16)] * NQ,
            *[pltpu.VMEM((512, 4, 128), BF16)] * NQ,
        ],
        compiler_params=pltpu.CompilerParams(
            collective_id=0, has_side_effects=True, vmem_limit_bytes=48 * 1024 * 1024
        ),
        name="h2",
    )(*[pltpu.with_memory_space_constraint(a, pltpu.HBM) for a in args[:6] + tuple(v.T for v in args[6:])])


def solution(mesh):
    both = ("stream", "leaf")
    placed = tuple(P(both, *([None] * n)) for n in (2, 2, 2, 2, 2, 3, 1, 1, 1, 1))
    return jax.shard_map(
        on_device, mesh=mesh, in_specs=placed, out_specs=P(both, None, None), check_vma=False
    )
```
